512 devices in a mesh: prow: 32 (over z, y_hi), pcol: 16 (over y_lo, x, core).
Axes of the slice: x: 4, y: 4 (y_hi: 2, y_lo: 2; y = y_hi * 2 + y_lo), z: 16, core: 2. Of those that a mesh axis runs over, the one named last changes fastest.
Arguments:
- matrix: float32 [8192, 8192], P('prow', 'pcol'), as said below
Outputs:
- complement: float32 [8192, 8192], P('prow', 'pcol')
- panel_columns: float32 [8192, 512], P(('prow', 'pcol'))
- pivot_values: float32 [512], replicated
Inputs may be any that keep to these rules, and one draw needn't show every extreme that they name: matrix is symmetric and positive definite, with its smallest eigenvalue above a six-hundredth of its largest diagonal entry.
All inputs are finite; a program needn't handle non-finite values.
Results may differ from the reference program's by a relative error of at most 0.00014.
Values sent between devices are 32-bit elements; how exact they have to be, the bound alone decides.
No kernel may reach another device: no remote copies, remote signals or barrier semaphores. Data moves between devices by JAX's collectives and lax.ppermute only.
A program may use at most 128 MiB of HBM per device.

```python
import math
import jax
import jax.numpy as jnp
from jax import lax

NB = 256
PANELS = 2
ORDER = 8192


def draw_matrix(key, part):
    base = jax.random.fold_in(key, 17)
    first_key, second_key, third_key = jax.random.split(base, 3)
    points = jax.random.uniform(first_key, (ORDER, 3), jnp.float32, 0.0, 1.0)
    angles = jax.random.uniform(second_key, (ORDER,), jnp.float32, -math.pi, math.pi)
    rescale = jnp.exp(jax.random.uniform(third_key, (ORDER,), jnp.float32, math.log(0.6), math.log(1.6)))
    reach = (0.764 / (PANELS * NB)) ** (1.0 / 3.0)
    first_gap = points[:, None, 0] - points[None, :, 0]
    second_gap = points[:, None, 1] - points[None, :, 1]
    third_gap = points[:, None, 2] - points[None, :, 2]
    distance = jnp.sqrt(first_gap * first_gap + second_gap * second_gap + third_gap * third_gap)
    kernel = jnp.exp(-distance / reach)
    cosine = jnp.cos(angles)
    sine = jnp.sin(angles)
    phase = cosine[:, None] * cosine[None, :] + sine[:, None] * sine[None, :]
    index_rows = jnp.arange(ORDER).astype(jnp.int32)
    lifted = jnp.where(index_rows[:, None] == index_rows[None, :], jnp.float32(0.25), jnp.float32(0.0))
    core = kernel * phase + lifted
    outer = rescale[:, None] * rescale[None, :]
    return (core * outer).astype(jnp.float32)


def setup_inputs(seed: int = 0) -> dict:
    splits = jax.random.split(jax.random.key(seed), 2)
    matrix = draw_matrix(jax.random.fold_in(splits[1], 71), 0)
    return dict(matrix=matrix)


def reference(matrix):
    current = matrix
    position = jnp.arange(ORDER).astype(jnp.int32)
    column_list = []
    pivot_list = []
    for panel in range(PANELS):
        first = panel * NB
        diagonal = current[first:first + NB, first:first + NB]
        cholesky_factor = jnp.linalg.cholesky(diagonal)
        scaling = jnp.diagonal(cholesky_factor)
        identity = jnp.eye(NB, dtype=current.dtype)
        inverse = jax.scipy.linalg.solve_triangular(cholesky_factor, identity, lower=True)
        projected = jnp.dot(current[:, first:first + NB], inverse.T, precision=lax.Precision.HIGHEST)
        factored = projected * scaling
        pivot = scaling * scaling
        weighed = factored / pivot
        current = current - jnp.dot(weighed, factored.T, precision=lax.Precision.HIGHEST)
        retained = position >= first + NB
        current = jnp.where(retained[:, None] & retained[None, :], current, jnp.zeros_like(current))
        column_list.append(factored)
        pivot_list.append(pivot)
    return (current, jnp.concatenate(column_list, axis=1), jnp.concatenate(pivot_list))
```

```python
import jax
import jax.numpy as jnp
from jax import lax
from jax.experimental import pallas as pl
from jax.experimental.pallas import tpu as pltpu
from jax.sharding import Mesh
from jax.sharding import PartitionSpec as P

NB = 256
PANELS = 2
WIDTH = NB * PANELS
BLOCK = 128
STEP = 8
PROW = ("z", "yh")
HIGHEST = lax.Precision.HIGHEST


def product(left, right, left_axis, right_axis):
    return lax.dot_general(
        left,
        right,
        (((left_axis,), (right_axis,)), ((), ())),
        precision=HIGHEST,
        preferred_element_type=jnp.float32,
    )


def factor_block(work, inverse, scaled, base):
    sublane = lax.broadcasted_iota(jnp.int32, (STEP, BLOCK), 0)

    def spread_row(value, index):
        return jnp.broadcast_to(value[index : index + 1, :], (STEP, BLOCK))

    def spread_column(value, index):
        return jnp.broadcast_to(value[:, index : index + 1], (STEP, BLOCK))

    steps = BLOCK // STEP
    for step in range(steps):
        at = STEP * step
        ahead = step < steps - 1
        rows = work[base + at : base + at + STEP, base : base + BLOCK]
        turned = inverse[at : at + STEP, :]
        columns = [spread_column(rows, at + j) for j in range(STEP)]
        if ahead:
            next_rows = work[base + at + STEP : base + at + 2 * STEP, base : base + BLOCK]
            next_turned = inverse[at + STEP : at + 2 * STEP, :]
            next_columns = [spread_column(next_rows, at + j) for j in range(STEP)]
        reciprocals = jnp.zeros((STEP, BLOCK), jnp.float32)
        for k in range(STEP):
            reciprocal = 1.0 / spread_row(columns[k], k)
            factor = jnp.where(sublane > k, columns[k] * reciprocal, 0.0)
            if ahead:
                next_factor = next_columns[k] * reciprocal
            for j in range(k + 1, STEP):
                pivot_entry = spread_row(columns[j], k)
                columns[j] = columns[j] - factor * pivot_entry
                if ahead:
                    next_columns[j] = next_columns[j] - next_factor * pivot_entry
            pivot_row = spread_row(rows, k)
            pivot_turned = spread_row(turned, k)
            rows = rows - factor * pivot_row
            turned = turned - factor * pivot_turned
            if ahead:
                next_rows = next_rows - next_factor * pivot_row
                next_turned = next_turned - next_factor * pivot_turned
            reciprocals = jnp.where(sublane == k, reciprocal, reciprocals)
        work[base + at : base + at + STEP, base : base + BLOCK] = rows
        inverse[at : at + STEP, :] = turned
        scaled[at : at + STEP, :] = turned * reciprocals
        if ahead:
            work[base + at + STEP : base + at + 2 * STEP, base : base + BLOCK] = next_rows
            inverse[at + STEP : at + 2 * STEP, :] = next_turned
        if step < steps - 2:
            later = at + 2 * STEP
            change = product(rows * reciprocals, jnp.concatenate([rows, turned], axis=1), 0, 0)
            work[base + later : base + BLOCK, base : base + BLOCK] = (
                work[base + later : base + BLOCK, base : base + BLOCK] - change[later:, :BLOCK]
            )
            inverse[later:, :] = inverse[later:, :] - change[later:, BLOCK:]


def factor_kernel(place, gathered, other, inverse, pivots, work, block_inverse, block_scaled):
    own = gathered[:, 16:32, :].reshape(NB, WIDTH)

    @pl.when(place[0] == 0)
    def _():
        work[:NB, :] = own
        work[NB:, :NB] = own[:, NB:].T
        work[NB:, NB:] = other[...]

    @pl.when(place[0] == 1)
    def _():
        work[NB:, :] = own
        work[:NB, NB:] = own[:, :NB].T
        work[:NB, :NB] = other[...]

    inverse[...] = jnp.zeros((WIDTH, WIDTH), jnp.float32)
    diagonal = lax.broadcasted_iota(jnp.int32, (BLOCK, BLOCK), 0) == lax.broadcasted_iota(
        jnp.int32, (BLOCK, BLOCK), 1
    )
    for base in range(0, WIDTH, BLOCK):
        end = base + BLOCK
        block_inverse[...] = diagonal.astype(jnp.float32)
        factor_block(work, block_inverse, block_scaled, base)
        pivots[:, base:end] = jnp.sum(
            jnp.where(diagonal, work[base:end, base:end], 0.0), axis=0, keepdims=True
        )
        if end < WIDTH:
            right = product(block_scaled[...], work[base:end, end:], 1, 0)
            left = product(work[end:, base:end], block_inverse[...], 1, 1)
            work[end:, end:] = work[end:, end:] - product(left, right, 1, 0)
        if base > 0:
            scaled_rows = product(block_scaled[...], inverse[base:end, :base], 1, 0)
            inverse[base:end, :base] = product(
                block_inverse[...], inverse[base:end, :base], 1, 0
            )
        inverse[base:end, base:end] = block_inverse[...]
        if end < WIDTH:
            if base > 0:
                inverse[end:, :base] = inverse[end:, :base] - product(left, scaled_rows, 1, 0)
            inverse[end:, base:end] = inverse[end:, base:end] - product(
                left, block_scaled[...], 1, 0
            )


def apply_kernel(place, matrix, gathered, other, inverse, pivots, complement, panel, scratch):
    half, row_block, col_block = place[0], place[1], place[2]
    factored = product(gathered[:, 32:48, :].reshape(NB, WIDTH), inverse[...], 1, 1)
    lane = lax.broadcasted_iota(jnp.int32, (NB, WIDTH), 1)
    scratch[...] = jnp.where((row_block == 0) & (lane >= NB), 0.0, factored)
    panel[...] = scratch[pl.ds(pl.multiple_of(16 * col_block, 16), 16), :]
    weighed = product(factored / pivots[...], inverse[...], 1, 0)
    kept = (row_block >= PANELS) & (col_block >= 1)
    first = pl.ds(pl.multiple_of(NB * half, NB), NB)
    second = pl.ds(pl.multiple_of(NB * (1 - half), NB), NB)
    change = product(weighed, gathered[:, :16, :].reshape(NB, WIDTH), 1, 1)
    complement[:, first] = jnp.where(kept, matrix[:, first] - change, 0.0)
    change = product(weighed, other[...], 1, 1)
    complement[:, second] = jnp.where(kept, matrix[:, second] - change, 0.0)


def on_device(matrix):
    half = lax.axis_index("yh")
    row_block = lax.axis_index(PROW)
    col_block = lax.axis_index("pcol")
    place = jnp.stack([half, row_block, col_block]).astype(jnp.int32)
    columns = lax.axis_size("pcol")
    scattered = lax.all_to_all(
        matrix.reshape(columns, -1, WIDTH), "pcol", 0, 0, tiled=True
    )[0]
    along = lax.all_gather(scattered, "z")
    packed = jnp.concatenate(
        [
            along,
            jnp.broadcast_to(along[:1], along.shape),
            jnp.broadcast_to(scattered[None], along.shape),
        ],
        axis=1,
    )
    gathered = lax.all_to_all(packed, "pcol", 0, 0, tiled=True)
    swap = [(0, 1), (1, 0)]
    corner = lax.dynamic_slice_in_dim(
        gathered[:, 16:32, :].reshape(NB, WIDTH), half * NB, NB, axis=1
    )
    other_corner = lax.ppermute(corner, "yh", swap)
    columns_half, other_corner = lax.optimization_barrier(
        (gathered[:, :16, :].reshape(NB, WIDTH), other_corner)
    )
    other_columns = lax.ppermute(columns_half, "yh", swap)
    smem = pl.BlockSpec(memory_space=pltpu.SMEM)
    vmem = pl.BlockSpec(memory_space=pltpu.VMEM)
    inverse, pivots = pl.pallas_call(
        factor_kernel,
        out_shape=(
            jax.ShapeDtypeStruct((WIDTH, WIDTH), jnp.float32),
            jax.ShapeDtypeStruct((1, WIDTH), jnp.float32),
        ),
        in_specs=[smem, vmem, vmem],
        out_specs=(vmem, vmem),
        scratch_shapes=[
            pltpu.VMEM((WIDTH, WIDTH), jnp.float32),
            pltpu.VMEM((BLOCK, BLOCK), jnp.float32),
            pltpu.VMEM((BLOCK, BLOCK), jnp.float32),
        ],
        cost_estimate=pl.CostEstimate(
            flops=200_000_000, bytes_accessed=3_000_000, transcendentals=0
        ),
        name="factor",
    )(place, gathered, other_corner)
    complement, panel = pl.pallas_call(
        apply_kernel,
        out_shape=(
            jax.ShapeDtypeStruct(matrix.shape, jnp.float32),
            jax.ShapeDtypeStruct((16, WIDTH), jnp.float32),
        ),
        in_specs=[smem, vmem, vmem, vmem, vmem, vmem],
        out_specs=(vmem, vmem),
        scratch_shapes=[pltpu.VMEM((NB, WIDTH), jnp.float32)],
        cost_estimate=pl.CostEstimate(
            flops=400_000_000, bytes_accessed=5_000_000, transcendentals=0
        ),
        name="apply",
    )(place, matrix, gathered, other_columns, inverse, pivots)
    return complement, panel, pivots.reshape(WIDTH)


def solution(mesh):
    split = Mesh(mesh.devices.reshape(16, 2, mesh.shape["pcol"]), ("z", "yh", "pcol"))
    return jax.shard_map(
        on_device,
        mesh=split,
        in_specs=(P(PROW, "pcol"),),
        out_specs=(P(PROW, "pcol"), P((*PROW, "pcol"), None), P()),
        check_vma=False,
    )
```

```python
import jax
import jax.numpy as jnp
from jax import lax
from jax.experimental import pallas as pl
from jax.experimental.pallas import tpu as pltpu
from jax.sharding import Mesh
from jax.sharding import PartitionSpec as P

NB = 256
PANELS = 2
WIDTH = NB * PANELS
BLOCK = 128
STEP = 8
PROW = ("z", "yh")
HIGHEST = lax.Precision.HIGHEST


def product(left, right, left_axis, right_axis):
    return lax.dot_general(
        left,
        right,
        (((left_axis,), (right_axis,)), ((), ())),
        precision=HIGHEST,
        preferred_element_type=jnp.float32,
    )


def split(value):
    high = value.astype(jnp.bfloat16).astype(jnp.float32)
    rest = value - high
    middle = rest.astype(jnp.bfloat16).astype(jnp.float32)
    return high, middle, rest - middle


def factor_block(block, reciprocals_out):
    sublane = lax.broadcasted_iota(jnp.int32, (STEP, BLOCK), 0)
    lane = lax.broadcasted_iota(jnp.int32, (STEP, BLOCK), 1)

    def spread_row(value, index):
        return jnp.broadcast_to(value[index : index + 1, :], (STEP, BLOCK))

    def spread_column(value, index):
        return jnp.broadcast_to(value[:, index : index + 1], (STEP, BLOCK))

    pivots = jnp.zeros((STEP, BLOCK), jnp.float32)
    steps = BLOCK // STEP
    columns = None
    for step in range(steps):
        at = STEP * step
        ahead = step < steps - 1
        current = (lane >= at) & (lane < at + STEP)
        rows = block[at : at + STEP, :]
        if columns is None:
            columns = [spread_column(rows, at + j) for j in range(STEP)]
        rows = jnp.where(current, jnp.where(lane == sublane + at, 1.0, 0.0), rows)
        if ahead:
            next_rows = block[at + STEP : at + 2 * STEP, :]
            below = [spread_column(next_rows, at + j) for j in range(STEP)]
            upcoming = [spread_column(next_rows, at + STEP + j) for j in range(STEP)]
            next_rows = jnp.where(current, 0.0, next_rows)
        reciprocals = jnp.zeros((STEP, BLOCK), jnp.float32)
        for k in range(STEP):
            pivot = spread_row(columns[k], k)
            reciprocal = 1.0 / pivot
            factor = jnp.where(sublane > k, columns[k] * reciprocal, 0.0)
            for j in range(k + 1, STEP):
                columns[j] = columns[j] - factor * spread_row(columns[j], k)
            pivot_row = spread_row(rows, k)
            rows = rows - factor * pivot_row
            if ahead:
                below_factor = below[k] * reciprocal
                for j in range(STEP):
                    upcoming[j] = upcoming[j] - below_factor * spread_row(below[k], j)
                for j in range(k + 1, STEP):
                    below[j] = below[j] - below[k] * spread_row(factor, j)
                next_rows = next_rows - below_factor * pivot_row
            reciprocals = jnp.where(sublane == k, reciprocal, reciprocals)
            pivots = jnp.where(lane == at + k, pivot, pivots)
        block[at : at + STEP, :] = rows
        reciprocals_out[at : at + STEP, :] = reciprocals
        if ahead:
            block[at + STEP : at + 2 * STEP, :] = next_rows
            columns = upcoming
        if step < steps - 2:
            later = at + 2 * STEP
            a, b, c = split(rows * reciprocals)
            d, e, f = split(rows)
            change = lax.dot_general(
                jnp.concatenate([a, a, b, b, a, c], axis=0),
                jnp.concatenate([d, e, d, e, f, d], axis=0),
                (((0,), (0,)), ((), ())),
                preferred_element_type=jnp.float32,
            )
            lanes = lax.broadcasted_iota(jnp.int32, (BLOCK - later, BLOCK), 1)
            block[later:, :] = (
                jnp.where((lanes >= at) & (lanes < at + STEP), 0.0, block[later:, :])
                - change[later:, :]
            )
    return pivots[:1, :]


def factor_kernel(gathered, inverse, pivots, work, block, reciprocals):
    half, quarter = NB, BLOCK
    work[:half, :half] = gathered[:16, :, :half].reshape(NB, NB)
    work[half:, half:] = gathered[16:, :, :half].reshape(NB, NB)
    work[half + quarter :, :quarter] = gathered[:8, :, half:].reshape(BLOCK, BLOCK).T
    work[half : half + quarter, quarter:half] = gathered[8:16, :, half:].reshape(BLOCK, BLOCK).T
    work[half : half + quarter, :quarter] = gathered[16:24, :, half:].reshape(BLOCK, BLOCK)
    work[half + quarter :, quarter:half] = gathered[24:, :, half:].reshape(BLOCK, BLOCK)
    inverse[...] = jnp.zeros((WIDTH, WIDTH), jnp.float32)
    lower = lax.broadcasted_iota(jnp.int32, (BLOCK, BLOCK), 0) >= lax.broadcasted_iota(
        jnp.int32, (BLOCK, BLOCK), 1
    )
    for base in range(0, WIDTH, BLOCK):
        end = base + BLOCK
        block[...] = work[base:end, base:end]
        block_pivots = factor_block(block, reciprocals)
        pivots[:, base:end] = block_pivots
        turned = jnp.where(lower, block[...], 0.0)
        scaled = turned * reciprocals[...]
        if end < WIDTH:
            left = product(work[end:, base:end], turned, 1, 1)
            weighed = left / block_pivots
            for at in range(end, WIDTH, BLOCK):
                work[at:, at : at + BLOCK] = work[at:, at : at + BLOCK] - product(
                    left[at - end :], weighed[at - end : at - end + BLOCK], 1, 1
                )
        if base > 0:
            scaled_rows = product(scaled, inverse[base:end, :base], 1, 0)
            inverse[base:end, :base] = product(turned, inverse[base:end, :base], 1, 0)
        inverse[base:end, base:end] = turned
        if end < WIDTH:
            if base > 0:
                inverse[end:, :base] = inverse[end:, :base] - product(left, scaled_rows, 1, 0)
            inverse[end:, base:end] = inverse[end:, base:end] - product(left, scaled, 1, 0)


def apply_kernel(place, matrix, own, across, inverse, pivots, complement, panel, scratch):
    row_block, col_block = place[0], place[1]
    factored = product(own[...].reshape(NB, WIDTH), inverse[...], 1, 1)
    lane = lax.broadcasted_iota(jnp.int32, (NB, WIDTH), 1)
    scratch[...] = jnp.where((row_block == 0) & (lane >= NB), 0.0, factored)
    panel[...] = scratch[pl.ds(pl.multiple_of(16 * col_block, 16), 16), :]
    weighed = product(factored / pivots[...], inverse[...], 1, 0)
    kept = (row_block >= PANELS) & (col_block >= 1)
    change = product(weighed, across[...].reshape(WIDTH, WIDTH), 1, 1)
    complement[...] = jnp.where(kept, matrix[...] - change, 0.0)


def on_device(matrix):
    half = lax.axis_index("yh")
    row_block = lax.axis_index(PROW)
    col_block = lax.axis_index("pcol")
    place = jnp.stack([row_block, col_block]).astype(jnp.int32)
    columns = lax.axis_size("pcol")
    plane = ("yh", "pcol")
    scattered = lax.all_to_all(
        matrix.reshape(columns, -1, WIDTH), "pcol", 0, 0, tiled=True
    )[0]
    copies = jnp.broadcast_to(scattered[None], (columns, *scattered.shape))
    own = lax.all_to_all(copies, "pcol", 0, 0, tiled=True)
    along = lax.all_gather(scattered, "z")
    corner = along[0]
    upper = col_block >= columns // 2
    diagonal = jnp.where(half == 0, corner[:, :NB], corner[:, NB:])
    mine = jnp.where(
        half == 0,
        jnp.where(upper, corner[:, NB : NB + BLOCK], corner[:, NB + BLOCK :]),
        jnp.where(upper, corner[:, BLOCK:NB], corner[:, :BLOCK]),
    )
    piece = jnp.concatenate([diagonal, mine], axis=1)
    gathered = lax.all_to_all(
        jnp.broadcast_to(piece[None], (2 * columns, *piece.shape)), plane, 0, 0, tiled=True
    )
    across = lax.all_to_all(jnp.concatenate([along, along], axis=0), plane, 0, 0, tiled=True)
    smem = pl.BlockSpec(memory_space=pltpu.SMEM)
    vmem = pl.BlockSpec(memory_space=pltpu.VMEM)
    inverse, pivots = pl.pallas_call(
        factor_kernel,
        out_shape=(
            jax.ShapeDtypeStruct((WIDTH, WIDTH), jnp.float32),
            jax.ShapeDtypeStruct((1, WIDTH), jnp.float32),
        ),
        in_specs=[vmem],
        out_specs=(vmem, vmem),
        scratch_shapes=[
            pltpu.VMEM((WIDTH, WIDTH), jnp.float32),
            pltpu.VMEM((BLOCK, BLOCK), jnp.float32),
            pltpu.VMEM((BLOCK, BLOCK), jnp.float32),
        ],
        cost_estimate=pl.CostEstimate(
            flops=200_000_000, bytes_accessed=3_000_000, transcendentals=0
        ),
        name="factor",
    )(gathered)
    complement, panel = pl.pallas_call(
        apply_kernel,
        out_shape=(
            jax.ShapeDtypeStruct(matrix.shape, jnp.float32),
            jax.ShapeDtypeStruct((16, WIDTH), jnp.float32),
        ),
        in_specs=[smem, vmem, vmem, vmem, vmem, vmem],
        out_specs=(vmem, vmem),
        scratch_shapes=[pltpu.VMEM((NB, WIDTH), jnp.float32)],
        cost_estimate=pl.CostEstimate(
            flops=400_000_000, bytes_accessed=5_000_000, transcendentals=0
        ),
        name="apply",
    )(place, matrix, own, across, inverse, pivots)
    return complement, panel, pivots.reshape(WIDTH)


def solution(mesh):
    split = Mesh(mesh.devices.reshape(16, 2, mesh.shape["pcol"]), ("z", "yh", "pcol"))
    return jax.shard_map(
        on_device,
        mesh=split,
        in_specs=(P(PROW, "pcol"),),
        out_specs=(P(PROW, "pcol"), P((*PROW, "pcol"), None), P()),
        check_vma=False,
    )
```

```python
import jax
import jax.numpy as jnp
from jax import lax
from jax.experimental import pallas as pl
from jax.experimental.pallas import tpu as pltpu
from jax.sharding import Mesh
from jax.sharding import PartitionSpec as P

NB = 256
PANELS = 2
WIDTH = NB * PANELS
BLOCK = 128
STEP = 8
PROW = ("z", "yh")
HIGHEST = lax.Precision.HIGHEST


def product(left, right, left_axis, right_axis):
    return lax.dot_general(
        left,
        right,
        (((left_axis,), (right_axis,)), ((), ())),
        precision=HIGHEST,
        preferred_element_type=jnp.float32,
    )


def split(value):
    high = value.astype(jnp.bfloat16).astype(jnp.float32)
    rest = value - high
    middle = rest.astype(jnp.bfloat16).astype(jnp.float32)
    return high, middle, rest - middle


def factor_block(block, reciprocals_out):
    sublane = lax.broadcasted_iota(jnp.int32, (STEP, BLOCK), 0)
    lane = lax.broadcasted_iota(jnp.int32, (STEP, BLOCK), 1)

    def spread_row(value, index):
        return jnp.broadcast_to(value[index : index + 1, :], (STEP, BLOCK))

    def spread_column(value, index):
        return jnp.broadcast_to(value[:, index : index + 1], (STEP, BLOCK))

    pivots = jnp.zeros((STEP, BLOCK), jnp.float32)
    steps = BLOCK // STEP
    columns = None
    for step in range(steps):
        at = STEP * step
        ahead = step < steps - 1
        current = (lane >= at) & (lane < at + STEP)
        rows = block[at : at + STEP, :]
        if columns is None:
            columns = [spread_column(rows, at + j) for j in range(STEP)]
        rows = jnp.where(current, jnp.where(lane == sublane + at, 1.0, 0.0), rows)
        if ahead:
            next_rows = block[at + STEP : at + 2 * STEP, :]
            below = [spread_column(next_rows, at + j) for j in range(STEP)]
            upcoming = [spread_column(next_rows, at + STEP + j) for j in range(STEP)]
            next_rows = jnp.where(current, 0.0, next_rows)
        reciprocals = jnp.zeros((STEP, BLOCK), jnp.float32)
        for k in range(STEP):
            pivot = spread_row(columns[k], k)
            reciprocal = 1.0 / pivot
            factor = jnp.where(sublane > k, columns[k] * reciprocal, 0.0)
            for j in range(k + 1, STEP):
                columns[j] = columns[j] - factor * spread_row(columns[j], k)
            pivot_row = spread_row(rows, k)
            rows = rows - factor * pivot_row
            if ahead:
                below_factor = below[k] * reciprocal
                for j in range(STEP):
                    upcoming[j] = upcoming[j] - below_factor * spread_row(below[k], j)
                for j in range(k + 1, STEP):
                    below[j] = below[j] - below[k] * spread_row(factor, j)
                next_rows = next_rows - below_factor * pivot_row
            reciprocals = jnp.where(sublane == k, reciprocal, reciprocals)
            pivots = jnp.where(lane == at + k, pivot, pivots)
        block[at : at + STEP, :] = rows
        reciprocals_out[at : at + STEP, :] = reciprocals
        if ahead:
            block[at + STEP : at + 2 * STEP, :] = next_rows
            columns = upcoming
        if step < steps - 2:
            later = at + 2 * STEP
            a, b, c = split(rows * reciprocals)
            d, e, f = split(rows)
            change = lax.dot_general(
                jnp.concatenate([a, a, b, b, a, c], axis=0),
                jnp.concatenate([d, e, d, e, f, d], axis=0),
                (((0,), (0,)), ((), ())),
                preferred_element_type=jnp.float32,
            )
            lanes = lax.broadcasted_iota(jnp.int32, (BLOCK - later, BLOCK), 1)
            block[later:, :] = (
                jnp.where((lanes >= at) & (lanes < at + STEP), 0.0, block[later:, :])
                - change[later:, :]
            )
    return pivots[:1, :]


def factor_kernel(gathered, inverse, pivots, work, block, reciprocals):
    half, quarter = NB, BLOCK
    work[:half, :half] = gathered[:16, :, :half].reshape(NB, NB)
    work[half:, half:] = gathered[16:, :, :half].reshape(NB, NB)
    work[half + quarter :, :quarter] = gathered[:8, :, half:].reshape(BLOCK, BLOCK).T
    work[half : half + quarter, quarter:half] = gathered[8:16, :, half:].reshape(BLOCK, BLOCK).T
    work[half : half + quarter, :quarter] = gathered[16:24, :, half:].reshape(BLOCK, BLOCK)
    work[half + quarter :, quarter:half] = gathered[24:, :, half:].reshape(BLOCK, BLOCK)
    inverse[...] = jnp.zeros((WIDTH, WIDTH), jnp.float32)
    lower = lax.broadcasted_iota(jnp.int32, (BLOCK, BLOCK), 0) >= lax.broadcasted_iota(
        jnp.int32, (BLOCK, BLOCK), 1
    )
    for base in range(0, WIDTH, BLOCK):
        end = base + BLOCK
        block[...] = work[base:end, base:end]
        block_pivots = factor_block(block, reciprocals)
        pivots[:, base:end] = block_pivots
        turned = jnp.where(lower, block[...], 0.0)
        scaled = turned * reciprocals[...]
        if end < WIDTH:
            left = product(work[end:, base:end], turned, 1, 1)
            weighed = left / block_pivots
            for at in range(end, WIDTH, BLOCK):
                work[at:, at : at + BLOCK] = work[at:, at : at + BLOCK] - product(
                    left[at - end :], weighed[at - end : at - end + BLOCK], 1, 1
                )
        if base > 0:
            scaled_rows = product(scaled, inverse[base:end, :base], 1, 0)
            inverse[base:end, :base] = product(turned, inverse[base:end, :base], 1, 0)
        inverse[base:end, base:end] = turned
        if end < WIDTH:
            if base > 0:
                inverse[end:, :base] = inverse[end:, :base] - product(left, scaled_rows, 1, 0)
            inverse[end:, base:end] = inverse[end:, base:end] - product(left, scaled, 1, 0)


def apply_kernel(
    place, matrix, own, across, inverse, pivots, complement, panel, factored, weighed, local, arrived
):
    fetch = pltpu.make_async_copy(matrix, local, arrived)
    fetch.start()
    row_block, col_block = place[0], place[1]
    rows = own[...].reshape(NB, WIDTH)
    for base in range(0, WIDTH, BLOCK):
        end = base + BLOCK
        part = product(rows[:, :end], inverse[base:end, :end], 1, 1)
        weighed[:, base:end] = part / pivots[:, base:end]
        if base >= NB:
            part = jnp.where(row_block == 0, 0.0, part)
        factored[:, base:end] = part
    panel[...] = factored[pl.ds(pl.multiple_of(16 * col_block, 16), 16), :]
    turned = jnp.concatenate(
        [
            product(weighed[:, base:], inverse[base:, base : base + BLOCK], 1, 0)
            for base in range(0, WIDTH, BLOCK)
        ],
        axis=1,
    )
    change = product(turned, across[...].reshape(WIDTH, WIDTH), 1, 1)
    fetch.wait()
    kept = (row_block >= PANELS) & (col_block >= 1)
    complement[...] = jnp.where(kept, local[...] - change, 0.0)


def in_vmem(array):
    return pltpu.with_memory_space_constraint(array, pltpu.VMEM)


def on_device(matrix):
    half = lax.axis_index("yh")
    row_block = lax.axis_index(PROW)
    col_block = lax.axis_index("pcol")
    place = jnp.stack([row_block, col_block]).astype(jnp.int32)
    columns = lax.axis_size("pcol")
    plane = ("yh", "pcol")
    scattered = lax.all_to_all(
        matrix.reshape(columns, -1, WIDTH), "pcol", 0, 0, tiled=True
    )[0]
    copies = jnp.broadcast_to(scattered[None], (columns, *scattered.shape))
    own = lax.all_to_all(copies, "pcol", 0, 0, tiled=True)
    along = lax.all_gather(scattered, "z")
    corner = along[0]
    upper = col_block >= columns // 2
    diagonal = jnp.where(half == 0, corner[:, :NB], corner[:, NB:])
    mine = jnp.where(
        half == 0,
        jnp.where(upper, corner[:, NB : NB + BLOCK], corner[:, NB + BLOCK :]),
        jnp.where(upper, corner[:, BLOCK:NB], corner[:, :BLOCK]),
    )
    piece = jnp.concatenate([diagonal, mine], axis=1)
    gathered = lax.all_to_all(
        jnp.broadcast_to(piece[None], (2 * columns, *piece.shape)), plane, 0, 0, tiled=True
    )
    across = lax.all_to_all(jnp.concatenate([along, along], axis=0), plane, 0, 0, tiled=True)
    smem = pl.BlockSpec(memory_space=pltpu.SMEM)
    vmem = pl.BlockSpec(memory_space=pltpu.VMEM)
    inverse, pivots = pl.pallas_call(
        factor_kernel,
        out_shape=(
            pltpu.VMEM((WIDTH, WIDTH), jnp.float32),
            jax.ShapeDtypeStruct((1, WIDTH), jnp.float32),
        ),
        in_specs=[vmem],
        out_specs=(vmem, vmem),
        scratch_shapes=[
            pltpu.VMEM((WIDTH, WIDTH), jnp.float32),
            pltpu.VMEM((BLOCK, BLOCK), jnp.float32),
            pltpu.VMEM((BLOCK, BLOCK), jnp.float32),
        ],
        cost_estimate=pl.CostEstimate(
            flops=200_000_000, bytes_accessed=3_000_000, transcendentals=0
        ),
        name="factor",
    )(in_vmem(gathered))
    complement, panel = pl.pallas_call(
        apply_kernel,
        out_shape=(
            jax.ShapeDtypeStruct(matrix.shape, jnp.float32),
            jax.ShapeDtypeStruct((16, WIDTH), jnp.float32),
        ),
        in_specs=[smem, pl.BlockSpec(memory_space=pl.ANY), vmem, vmem, vmem, vmem],
        out_specs=(vmem, vmem),
        scratch_shapes=[
            pltpu.VMEM((NB, WIDTH), jnp.float32),
            pltpu.VMEM((NB, WIDTH), jnp.float32),
            pltpu.VMEM((NB, WIDTH), jnp.float32),
            pltpu.SemaphoreType.DMA(()),
        ],
        cost_estimate=pl.CostEstimate(
            flops=400_000_000, bytes_accessed=5_000_000, transcendentals=0
        ),
        name="apply",
    )(place, matrix, in_vmem(own), in_vmem(across), in_vmem(inverse), pivots)
    return complement, panel, pivots.reshape(WIDTH)


def solution(mesh):
    split = Mesh(mesh.devices.reshape(16, 2, mesh.shape["pcol"]), ("z", "yh", "pcol"))
    return jax.shard_map(
        on_device,
        mesh=split,
        in_specs=(P(PROW, "pcol"),),
        out_specs=(P(PROW, "pcol"), P((*PROW, "pcol"), None), P()),
        check_vma=False,
    )
```

```python
import jax
import jax.numpy as jnp
from jax import lax
from jax.experimental import pallas as pl
from jax.experimental.pallas import tpu as pltpu
from jax.sharding import Mesh
from jax.sharding import PartitionSpec as P

NB = 256
PANELS = 2
WIDTH = NB * PANELS
BLOCK = 128
STEP = 8
PROW = ("z", "yh")
HIGHEST = lax.Precision.HIGHEST


def product(left, right, left_axis, right_axis):
    return lax.dot_general(
        left,
        right,
        (((left_axis,), (right_axis,)), ((), ())),
        precision=HIGHEST,
        preferred_element_type=jnp.float32,
    )


def split(value):
    high = value.astype(jnp.bfloat16).astype(jnp.float32)
    rest = value - high
    middle = rest.astype(jnp.bfloat16).astype(jnp.float32)
    return high, middle, rest - middle


def factor_block(block, reciprocals_out):
    sublane = lax.broadcasted_iota(jnp.int32, (STEP, BLOCK), 0)
    lane = lax.broadcasted_iota(jnp.int32, (STEP, BLOCK), 1)

    def spread_row(value, index):
        return jnp.broadcast_to(value[index : index + 1, :], (STEP, BLOCK))

    def spread_column(value, index):
        return jnp.broadcast_to(value[:, index : index + 1], (STEP, BLOCK))

    pivots = jnp.zeros((STEP, BLOCK), jnp.float32)
    steps = BLOCK // STEP
    columns = None
    for step in range(steps):
        at = STEP * step
        ahead = step < steps - 1
        current = (lane >= at) & (lane < at + STEP)
        rows = block[at : at + STEP, :]
        if columns is None:
            columns = [spread_column(rows, at + j) for j in range(STEP)]
        rows = jnp.where(current, jnp.where(lane == sublane + at, 1.0, 0.0), rows)
        if ahead:
            next_rows = block[at + STEP : at + 2 * STEP, :]
            below = [spread_column(next_rows, at + j) for j in range(STEP)]
            upcoming = [spread_column(next_rows, at + STEP + j) for j in range(STEP)]
            next_rows = jnp.where(current, 0.0, next_rows)
        reciprocals = jnp.zeros((STEP, BLOCK), jnp.float32)
        for k in range(STEP):
            pivot = spread_row(columns[k], k)
            reciprocal = 1.0 / pivot
            factor = jnp.where(sublane > k, columns[k] * reciprocal, 0.0)
            for j in range(k + 1, STEP):
                columns[j] = columns[j] - factor * spread_row(columns[j], k)
            pivot_row = spread_row(rows, k)
            rows = rows - factor * pivot_row
            if ahead:
                below_factor = below[k] * reciprocal
                for j in range(STEP):
                    upcoming[j] = upcoming[j] - below_factor * spread_row(below[k], j)
                for j in range(k + 1, STEP):
                    below[j] = below[j] - below[k] * spread_row(factor, j)
                next_rows = next_rows - below_factor * pivot_row
            reciprocals = jnp.where(sublane == k, reciprocal, reciprocals)
            pivots = jnp.where(lane == at + k, pivot, pivots)
        block[at : at + STEP, :] = rows
        reciprocals_out[at : at + STEP, :] = reciprocals
        if ahead:
            block[at + STEP : at + 2 * STEP, :] = next_rows
            columns = upcoming
        if step < steps - 2:
            later = at + 2 * STEP
            a, b, c = split(rows * reciprocals)
            d, e, f = split(rows)
            change = lax.dot_general(
                jnp.concatenate([a, a, b, b, a, c], axis=0),
                jnp.concatenate([d, e, d, e, f, d], axis=0),
                (((0,), (0,)), ((), ())),
                preferred_element_type=jnp.float32,
            )
            lanes = lax.broadcasted_iota(jnp.int32, (BLOCK - later, BLOCK), 1)
            block[later:, :] = (
                jnp.where((lanes >= at) & (lanes < at + STEP), 0.0, block[later:, :])
                - change[later:, :]
            )
    return pivots[:1, :]


def factor_kernel(
    place, gathered, own, turned_rows, pivots, panel, corner, work, inverse, factored, block, reciprocals
):
    row_block, col_block, odd = place[0], place[1], place[2]
    for at in range(0, 2 * 16, 2):
        for side in range(2):
            corner[16 * (at + side) : 16 * (at + side + 1), :] = gathered[
                at + jnp.where(odd == 1, 1 - side, side)
            ]
    half, quarter = NB, BLOCK
    work[:half, :half] = corner[:half, :half]
    work[half:, half:] = corner[half:, :half]
    work[half + quarter :, :quarter] = corner[:quarter, half:].T
    work[half : half + quarter, quarter:half] = corner[quarter:half, half:].T
    work[half : half + quarter, :quarter] = corner[half : half + quarter, half:]
    work[half + quarter :, quarter:half] = corner[half + quarter :, half:]
    inverse[...] = jnp.zeros((WIDTH, WIDTH), jnp.float32)
    turned_rows[...] = jnp.zeros((NB, WIDTH), jnp.float32)
    lower = lax.broadcasted_iota(jnp.int32, (BLOCK, BLOCK), 0) >= lax.broadcasted_iota(
        jnp.int32, (BLOCK, BLOCK), 1
    )
    rows = own[...].reshape(NB, WIDTH)
    for base in range(0, WIDTH, BLOCK):
        end = base + BLOCK
        block[...] = work[base:end, base:end]
        block_pivots = factor_block(block, reciprocals)
        pivots[:, base:end] = block_pivots
        turned = jnp.where(lower, block[...], 0.0)
        scaled = turned * reciprocals[...]
        if end < WIDTH:
            left = product(work[end:, base:end], turned, 1, 1)
            weighed = left / block_pivots
            for at in range(end, WIDTH, BLOCK):
                work[at:, at : at + BLOCK] = work[at:, at : at + BLOCK] - product(
                    left[at - end :], weighed[at - end : at - end + BLOCK], 1, 1
                )
        if base > 0:
            scaled_rows = product(scaled, inverse[base:end, :base], 1, 0)
            inverse[base:end, :base] = product(turned, inverse[base:end, :base], 1, 0)
        inverse[base:end, base:end] = turned
        if end < WIDTH:
            if base > 0:
                inverse[end:, :base] = inverse[end:, :base] - product(left, scaled_rows, 1, 0)
            inverse[end:, base:end] = inverse[end:, base:end] - product(left, scaled, 1, 0)
        part = product(rows[:, :end], inverse[base:end, :end], 1, 1)
        turned_rows[:, :end] = turned_rows[:, :end] + product(
            part / block_pivots, inverse[base:end, :end], 1, 0
        )
        if base >= NB:
            part = jnp.where(row_block == 0, 0.0, part)
        factored[:, base:end] = part
    panel[...] = factored[pl.ds(pl.multiple_of(16 * col_block, 16), 16), :]


def apply_kernel(place, matrix, across, turned_rows, complement, ordered, local, arrived):
    fetch = pltpu.make_async_copy(matrix, local, arrived)
    fetch.start()
    row_block, col_block, swapped = place[0], place[1], place[3]
    for at in range(0, 2 * 16, 2):
        for side in range(2):
            ordered[16 * (at + side) : 16 * (at + side + 1), :] = across[
                at + jnp.where(swapped == 1, 1 - side, side)
            ]
    change = product(turned_rows[...], ordered[...], 1, 1)
    fetch.wait()
    kept = (row_block >= PANELS) & (col_block >= 1)
    complement[...] = jnp.where(kept, local[...] - change, 0.0)


def in_vmem(array):
    return pltpu.with_memory_space_constraint(array, pltpu.VMEM)


def on_device(matrix):
    half = lax.axis_index("yh")
    row_block = lax.axis_index(PROW)
    col_block = lax.axis_index("pcol")
    depth = lax.axis_index("z")
    place = jnp.stack([row_block, col_block, depth % 2, (depth + col_block) % 2])
    place = place.astype(jnp.int32)
    columns = lax.axis_size("pcol")
    plane = ("yh", "pcol")
    scattered = lax.all_to_all(
        matrix.reshape(columns, -1, WIDTH), "pcol", 0, 0, tiled=True
    )[0]
    copies = jnp.broadcast_to(scattered[None], (columns, *scattered.shape))
    own = lax.all_to_all(copies, "pcol", 0, 0, tiled=True)
    along = lax.all_gather(
        scattered,
        ("z", "pcol"),
        axis_index_groups=[
            [z * columns + at + (z + side) % 2 for z in range(lax.axis_size("z"))]
            for at in range(0, columns, 2)
            for side in range(2)
        ],
    )
    corner = along[0]
    upper = col_block >= columns // 2
    diagonal = jnp.where(half == 0, corner[:, :NB], corner[:, NB:])
    mine = jnp.where(
        half == 0,
        jnp.where(upper, corner[:, NB : NB + BLOCK], corner[:, NB + BLOCK :]),
        jnp.where(upper, corner[:, BLOCK:NB], corner[:, :BLOCK]),
    )
    piece = jnp.concatenate([diagonal, mine], axis=1)
    gathered = lax.all_to_all(
        jnp.broadcast_to(piece[None], (2 * columns, *piece.shape)), plane, 0, 0, tiled=True
    )
    across = lax.all_to_all(jnp.concatenate([along, along], axis=0), plane, 0, 0, tiled=True)
    smem = pl.BlockSpec(memory_space=pltpu.SMEM)
    vmem = pl.BlockSpec(memory_space=pltpu.VMEM)
    turned_rows, pivots, panel = pl.pallas_call(
        factor_kernel,
        out_shape=(
            pltpu.VMEM((NB, WIDTH), jnp.float32),
            jax.ShapeDtypeStruct((1, WIDTH), jnp.float32),
            jax.ShapeDtypeStruct((16, WIDTH), jnp.float32),
        ),
        in_specs=[smem, vmem, vmem],
        out_specs=(vmem, vmem, vmem),
        scratch_shapes=[
            pltpu.VMEM((WIDTH, NB + BLOCK), jnp.float32),
            pltpu.VMEM((WIDTH, WIDTH), jnp.float32),
            pltpu.VMEM((WIDTH, WIDTH), jnp.float32),
            pltpu.VMEM((NB, WIDTH), jnp.float32),
            pltpu.VMEM((BLOCK, BLOCK), jnp.float32),
            pltpu.VMEM((BLOCK, BLOCK), jnp.float32),
        ],
        cost_estimate=pl.CostEstimate(
            flops=400_000_000, bytes_accessed=3_000_000, transcendentals=0
        ),
        name="factor",
    )(place, in_vmem(gathered), in_vmem(own))
    complement = pl.pallas_call(
        apply_kernel,
        out_shape=jax.ShapeDtypeStruct(matrix.shape, jnp.float32),
        in_specs=[smem, pl.BlockSpec(memory_space=pl.ANY), vmem, vmem],
        out_specs=vmem,
        scratch_shapes=[
            pltpu.VMEM((WIDTH, WIDTH), jnp.float32),
            pltpu.VMEM((NB, WIDTH), jnp.float32),
            pltpu.SemaphoreType.DMA(()),
        ],
        cost_estimate=pl.CostEstimate(
            flops=200_000_000, bytes_accessed=3_000_000, transcendentals=0
        ),
        name="apply",
    )(place, matrix, in_vmem(across), in_vmem(turned_rows))
    return complement, panel, pivots.reshape(WIDTH)


def solution(mesh):
    split = Mesh(mesh.devices.reshape(16, 2, mesh.shape["pcol"]), ("z", "yh", "pcol"))
    return jax.shard_map(
        on_device,
        mesh=split,
        in_specs=(P(PROW, "pcol"),),
        out_specs=(P(PROW, "pcol"), P((*PROW, "pcol"), None), P()),
        check_vma=False,
    )
```

```python
import functools

import jax
import jax.numpy as jnp
from jax import lax
from jax.experimental import pallas as pl
from jax.experimental.pallas import tpu as pltpu
from jax.sharding import Mesh
from jax.sharding import PartitionSpec as P

NB = 256
PANELS = 2
WIDTH = NB * PANELS
BLOCK = 128
STEP = 8
NEAR = 2
PROW = ("z", "yh")
HIGHEST = lax.Precision.HIGHEST


def product(left, right, left_axis, right_axis):
    return lax.dot_general(
        left,
        right,
        (((left_axis,), (right_axis,)), ((), ())),
        precision=HIGHEST,
        preferred_element_type=jnp.float32,
    )


def split(value):
    high = value.astype(jnp.bfloat16).astype(jnp.float32)
    rest = value - high
    middle = rest.astype(jnp.bfloat16).astype(jnp.float32)
    return high, middle, rest - middle


def factor_block(block, reciprocals_out, between):
    sublane = lax.broadcasted_iota(jnp.int32, (STEP, BLOCK), 0)
    lane = lax.broadcasted_iota(jnp.int32, (STEP, BLOCK), 1)

    def spread_row(value, index):
        return jnp.broadcast_to(value[index : index + 1, :], (STEP, BLOCK))

    def spread_column(value, index):
        return jnp.broadcast_to(value[:, index : index + 1], (STEP, BLOCK))

    pivots = jnp.zeros((STEP, BLOCK), jnp.float32)
    steps = BLOCK // STEP
    columns = None
    lefts, rights = [], []
    for step in range(steps):
        at = STEP * step
        even = step % 2 == 0
        near = range(1, min(NEAR + even, steps - 1 - step) + 1)
        current = (lane >= at) & (lane < at + STEP)
        rows = block[at : at + STEP, :]
        if columns is None:
            columns = [spread_column(rows, at + j) for j in range(STEP)]
        rows = jnp.where(current, jnp.where(lane == sublane + at, 1.0, 0.0), rows)
        next_rows, below, upcoming = {}, {}, []
        for group in near:
            next_rows[group] = block[at + STEP * group : at + STEP * (group + 1), :]
            below[group] = [spread_column(next_rows[group], at + j) for j in range(STEP)]
            if group == 1:
                upcoming = [spread_column(next_rows[1], at + STEP + j) for j in range(STEP)]
            next_rows[group] = jnp.where(current, 0.0, next_rows[group])
        reciprocals = jnp.zeros((STEP, BLOCK), jnp.float32)
        for k in range(STEP):
            pivot = spread_row(columns[k], k)
            reciprocal = 1.0 / pivot
            factor = jnp.where(sublane > k, columns[k] * reciprocal, 0.0)
            for j in range(k + 1, STEP):
                columns[j] = columns[j] - factor * spread_row(columns[j], k)
            pivot_row = spread_row(rows, k)
            rows = rows - factor * pivot_row
            for group in near:
                below_factor = below[group][k] * reciprocal
                if group == 1:
                    for j in range(STEP):
                        upcoming[j] = upcoming[j] - below_factor * spread_row(below[1][k], j)
                for j in range(k + 1, STEP):
                    below[group][j] = below[group][j] - below[group][k] * spread_row(factor, j)
                next_rows[group] = next_rows[group] - below_factor * pivot_row
            reciprocals = jnp.where(sublane == k, reciprocal, reciprocals)
            pivots = jnp.where(lane == at + k, pivot, pivots)
        block[at : at + STEP, :] = rows
        reciprocals_out[at : at + STEP, :] = reciprocals
        for group in near:
            block[at + STEP * group : at + STEP * (group + 1), :] = next_rows[group]
        columns = upcoming
        later = STEP * (step - step % 2 + 2 + NEAR)
        if later < BLOCK:
            a, b, c = split(rows * reciprocals)
            if even:
                rows = jnp.where((lane >= at + STEP) & (lane < at + 2 * STEP), 0.0, rows)
            d, e, f = split(rows)
            lefts += [a, a, b, b, a, c]
            rights += [d, e, d, e, f, d]
            if not even:
                change = lax.dot_general(
                    jnp.concatenate(lefts, axis=0),
                    jnp.concatenate(rights, axis=0),
                    (((0,), (0,)), ((), ())),
                    preferred_element_type=jnp.float32,
                )
                lefts, rights = [], []
                lanes = lax.broadcasted_iota(jnp.int32, (BLOCK - later, BLOCK), 1)
                block[later:, :] = (
                    jnp.where((lanes >= at - STEP) & (lanes < at + STEP), 0.0, block[later:, :])
                    - change[later:, :]
                )
        between()
    return pivots[:1, :]


def factor_kernel(
    place,
    gathered,
    own,
    turned_rows,
    pivots,
    panel,
    corner,
    work,
    inverse,
    factored,
    left,
    ahead,
    block,
    reciprocals,
):
    row_block, col_block, odd = place[0], place[1], place[2]
    for at in range(0, 2 * 16, 2):
        for side in range(2):
            corner[16 * (at + side) : 16 * (at + side + 1), :] = gathered[
                at + jnp.where(odd == 1, 1 - side, side)
            ]
    half, quarter = NB, BLOCK
    work[:half, :half] = corner[:half, :half]
    work[half:, half:] = corner[half:, :half]
    work[half + quarter :, :quarter] = corner[:quarter, half:].T
    work[half : half + quarter, quarter:half] = corner[quarter:half, half:].T
    work[half : half + quarter, :quarter] = corner[half : half + quarter, half:]
    work[half + quarter :, quarter:half] = corner[half + quarter :, half:]
    lower = lax.broadcasted_iota(jnp.int32, (BLOCK, BLOCK), 0) >= lax.broadcasted_iota(
        jnp.int32, (BLOCK, BLOCK), 1
    )
    queue = []

    def between():
        if queue:
            queue.pop(0)()

    def set_columns(at):
        columns = own[:, :, at : at + BLOCK].reshape(NB, BLOCK)
        if at > 0:
            for row in range(0, NB, BLOCK):
                ahead[row : row + BLOCK, :] = columns[row : row + BLOCK] + product(
                    own[row // 16 : (row + BLOCK) // 16, :, :at].reshape(BLOCK, at),
                    inverse[at : at + BLOCK, :at],
                    1,
                    1,
                )
        else:
            ahead[...] = columns

    def set_left(base, row, turned):
        left[row : row + BLOCK, :] = product(
            work[row : row + BLOCK, base : base + BLOCK], turned, 1, 1
        )

    def update_work(row, column, block_pivots):
        work[row : row + BLOCK, column : column + BLOCK] = work[
            row : row + BLOCK, column : column + BLOCK
        ] - product(
            left[row : row + BLOCK, :], left[column : column + BLOCK, :] / block_pivots, 1, 1
        )

    def update_inverse(base, row, scaled):
        multipliers = product(left[row : row + BLOCK, :], scaled, 1, 0)
        inverse[row : row + BLOCK, base : base + BLOCK] = -multipliers
        if base > 0:
            inverse[row : row + BLOCK, :base] = inverse[row : row + BLOCK, :base] - product(
                multipliers, inverse[base : base + BLOCK, :base], 1, 0
            )

    def set_factored(base, turned):
        part = product(ahead[...], turned, 1, 1)
        if base >= NB:
            part = jnp.where(row_block == 0, 0.0, part)
        factored[:, base : base + BLOCK] = part

    def set_turned_rows(base, scaled):
        weighed = product(factored[:, base : base + BLOCK], scaled, 1, 0)
        turned_rows[:, base : base + BLOCK] = weighed

    def add_turned_rows(base):
        turned_rows[:, :base] = turned_rows[:, :base] + product(
            turned_rows[:, base : base + BLOCK], inverse[base : base + BLOCK, :base], 1, 0
        )

    set_columns(0)
    for base in range(0, WIDTH, BLOCK):
        end = base + BLOCK
        block[...] = work[base:end, base:end]
        block_pivots = factor_block(block, reciprocals, between)
        while queue:
            between()
        pivots[:, base:end] = block_pivots
        turned = jnp.where(lower, block[...], 0.0)
        scaled = turned * reciprocals[...]
        if end < WIDTH:
            set_left(base, end, turned)
            update_work(end, end, block_pivots)
        queue.append(functools.partial(set_factored, base, turned))
        queue.append(functools.partial(set_turned_rows, base, scaled))
        if base > 0:
            queue.append(functools.partial(add_turned_rows, base))
        if end < WIDTH:
            queue.append(functools.partial(update_inverse, base, end, scaled))
        for row in range(end + BLOCK, WIDTH, BLOCK):
            queue.append(functools.partial(set_left, base, row, turned))
            for column in range(end, row + BLOCK, BLOCK):
                queue.append(functools.partial(update_work, row, column, block_pivots))
            queue.append(functools.partial(update_inverse, base, row, scaled))
        if end < WIDTH:
            queue.append(functools.partial(set_columns, end))
    while queue:
        between()
    panel[...] = factored[pl.ds(pl.multiple_of(16 * col_block, 16), 16), :]


def apply_kernel(place, matrix, across, turned_rows, complement, ordered, local, arrived):
    fetch = pltpu.make_async_copy(matrix, local, arrived)
    fetch.start()
    row_block, col_block, swapped = place[0], place[1], place[3]
    for at in range(0, 2 * 16, 2):
        for side in range(2):
            ordered[16 * (at + side) : 16 * (at + side + 1), :] = across[
                at + jnp.where(swapped == 1, 1 - side, side)
            ]
    change = product(turned_rows[...], ordered[...], 1, 1)
    fetch.wait()
    kept = (row_block >= PANELS) & (col_block >= 1)
    complement[...] = jnp.where(kept, local[...] - change, 0.0)


def in_vmem(array):
    return pltpu.with_memory_space_constraint(array, pltpu.VMEM)


def on_device(matrix):
    half = lax.axis_index("yh")
    row_block = lax.axis_index(PROW)
    col_block = lax.axis_index("pcol")
    depth = lax.axis_index("z")
    place = jnp.stack([row_block, col_block, depth % 2, (depth + col_block) % 2])
    place = place.astype(jnp.int32)
    columns = lax.axis_size("pcol")
    plane = ("yh", "pcol")
    scattered = lax.all_to_all(
        matrix.reshape(columns, -1, WIDTH), "pcol", 0, 0, tiled=True
    )[0]
    copies = jnp.broadcast_to(scattered[None], (columns, *scattered.shape))
    own = lax.all_to_all(copies, "pcol", 0, 0, tiled=True)
    along = lax.all_gather(
        scattered,
        ("z", "pcol"),
        axis_index_groups=[
            [z * columns + at + (z + side) % 2 for z in range(lax.axis_size("z"))]
            for at in range(0, columns, 2)
            for side in range(2)
        ],
    )
    corner = along[0]
    upper = col_block >= columns // 2
    diagonal = jnp.where(half == 0, corner[:, :NB], corner[:, NB:])
    mine = jnp.where(
        half == 0,
        jnp.where(upper, corner[:, NB : NB + BLOCK], corner[:, NB + BLOCK :]),
        jnp.where(upper, corner[:, BLOCK:NB], corner[:, :BLOCK]),
    )
    piece = jnp.concatenate([diagonal, mine], axis=1)
    gathered = lax.all_to_all(
        jnp.broadcast_to(piece[None], (2 * columns, *piece.shape)), plane, 0, 0, tiled=True
    )
    across = lax.all_to_all(jnp.concatenate([along, along], axis=0), plane, 0, 0, tiled=True)
    smem = pl.BlockSpec(memory_space=pltpu.SMEM)
    vmem = pl.BlockSpec(memory_space=pltpu.VMEM)
    turned_rows, pivots, panel = pl.pallas_call(
        factor_kernel,
        out_shape=(
            pltpu.VMEM((NB, WIDTH), jnp.float32),
            jax.ShapeDtypeStruct((1, WIDTH), jnp.float32),
            jax.ShapeDtypeStruct((16, WIDTH), jnp.float32),
        ),
        in_specs=[smem, vmem, vmem],
        out_specs=(vmem, vmem, vmem),
        scratch_shapes=[
            pltpu.VMEM((WIDTH, NB + BLOCK), jnp.float32),
            pltpu.VMEM((WIDTH, WIDTH), jnp.float32),
            pltpu.VMEM((WIDTH, WIDTH), jnp.float32),
            pltpu.VMEM((NB, WIDTH), jnp.float32),
            pltpu.VMEM((WIDTH, BLOCK), jnp.float32),
            pltpu.VMEM((NB, BLOCK), jnp.float32),
            pltpu.VMEM((BLOCK, BLOCK), jnp.float32),
            pltpu.VMEM((BLOCK, BLOCK), jnp.float32),
        ],
        cost_estimate=pl.CostEstimate(
            flops=400_000_000, bytes_accessed=3_000_000, transcendentals=0
        ),
        name="factor",
    )(place, in_vmem(gathered), in_vmem(own))
    complement = pl.pallas_call(
        apply_kernel,
        out_shape=jax.ShapeDtypeStruct(matrix.shape, jnp.float32),
        in_specs=[smem, pl.BlockSpec(memory_space=pl.ANY), vmem, vmem],
        out_specs=vmem,
        scratch_shapes=[
            pltpu.VMEM((WIDTH, WIDTH), jnp.float32),
            pltpu.VMEM((NB, WIDTH), jnp.float32),
            pltpu.SemaphoreType.DMA(()),
        ],
        cost_estimate=pl.CostEstimate(
            flops=200_000_000, bytes_accessed=3_000_000, transcendentals=0
        ),
        name="apply",
    )(place, matrix, in_vmem(across), in_vmem(turned_rows))
    return complement, panel, pivots.reshape(WIDTH)


def solution(mesh):
    split = Mesh(mesh.devices.reshape(16, 2, mesh.shape["pcol"]), ("z", "yh", "pcol"))
    return jax.shard_map(
        on_device,
        mesh=split,
        in_specs=(P(PROW, "pcol"),),
        out_specs=(P(PROW, "pcol"), P((*PROW, "pcol"), None), P()),
        check_vma=False,
    )
```

```python
import functools

import jax
import jax.numpy as jnp
from jax import lax
from jax.experimental import pallas as pl
from jax.experimental.pallas import tpu as pltpu
from jax.sharding import Mesh
from jax.sharding import PartitionSpec as P

NB = 256
PANELS = 2
WIDTH = NB * PANELS
BLOCK = 128
STEP = 8
NEAR = 2
PROW = ("z", "yh")
HIGHEST = lax.Precision.HIGHEST


def product(left, right, left_axis, right_axis):
    return lax.dot_general(
        left,
        right,
        (((left_axis,), (right_axis,)), ((), ())),
        precision=HIGHEST,
        preferred_element_type=jnp.float32,
    )


def split(value):
    high = value.astype(jnp.bfloat16).astype(jnp.float32)
    rest = value - high
    middle = rest.astype(jnp.bfloat16).astype(jnp.float32)
    return high, middle, rest - middle


def factor_block(block, reciprocals_out, between):
    sublane = lax.broadcasted_iota(jnp.int32, (STEP, BLOCK), 0)
    lane = lax.broadcasted_iota(jnp.int32, (STEP, BLOCK), 1)

    def spread_row(value, index):
        return jnp.broadcast_to(value[index : index + 1, :], (STEP, BLOCK))

    def spread_column(value, index):
        return jnp.broadcast_to(value[:, index : index + 1], (STEP, BLOCK))

    pivots = jnp.zeros((STEP, BLOCK), jnp.float32)
    steps = BLOCK // STEP
    columns = None
    lefts, rights = [], []
    for step in range(steps):
        at = STEP * step
        even = step % 2 == 0
        near = range(1, min(NEAR + even, steps - 1 - step) + 1)
        current = (lane >= at) & (lane < at + STEP)
        rows = block[at : at + STEP, :]
        if columns is None:
            columns = [spread_column(rows, at + j) for j in range(STEP)]
        rows = jnp.where(current, jnp.where(lane == sublane + at, 1.0, 0.0), rows)
        next_rows, below, upcoming = {}, {}, []
        for group in near:
            next_rows[group] = block[at + STEP * group : at + STEP * (group + 1), :]
            below[group] = [spread_column(next_rows[group], at + j) for j in range(STEP)]
            if group == 1:
                upcoming = [spread_column(next_rows[1], at + STEP + j) for j in range(STEP)]
            next_rows[group] = jnp.where(current, 0.0, next_rows[group])
        reciprocals = jnp.zeros((STEP, BLOCK), jnp.float32)
        for k in range(STEP):
            pivot = spread_row(columns[k], k)
            reciprocal = 1.0 / pivot
            factor = jnp.where(sublane > k, columns[k] * reciprocal, 0.0)
            for j in range(k + 1, STEP):
                columns[j] = columns[j] - factor * spread_row(columns[j], k)
            pivot_row = spread_row(rows, k)
            rows = rows - factor * pivot_row
            for group in near:
                below_factor = below[group][k] * reciprocal
                if group == 1:
                    for j in range(STEP):
                        upcoming[j] = upcoming[j] - below_factor * spread_row(below[1][k], j)
                for j in range(k + 1, STEP):
                    below[group][j] = below[group][j] - below[group][k] * spread_row(factor, j)
                next_rows[group] = next_rows[group] - below_factor * pivot_row
            reciprocals = jnp.where(sublane == k, reciprocal, reciprocals)
            pivots = jnp.where(lane == at + k, pivot, pivots)
        block[at : at + STEP, :] = rows
        reciprocals_out[at : at + STEP, :] = reciprocals
        for group in near:
            block[at + STEP * group : at + STEP * (group + 1), :] = next_rows[group]
        columns = upcoming
        later = STEP * (step - step % 2 + 2 + NEAR)
        if later < BLOCK:
            a, b, c = split(rows * reciprocals)
            if even:
                rows = jnp.where((lane >= at + STEP) & (lane < at + 2 * STEP), 0.0, rows)
            d, e, f = split(rows)
            lefts += [a, a, b, b, a, c]
            rights += [d, e, d, e, f, d]
            if not even:
                change = lax.dot_general(
                    jnp.concatenate(lefts, axis=0),
                    jnp.concatenate(rights, axis=0),
                    (((0,), (0,)), ((), ())),
                    preferred_element_type=jnp.float32,
                )
                lefts, rights = [], []
                lanes = lax.broadcasted_iota(jnp.int32, (BLOCK - later, BLOCK), 1)
                block[later:, :] = (
                    jnp.where((lanes >= at - STEP) & (lanes < at + STEP), 0.0, block[later:, :])
                    - change[later:, :]
                )
        between()
    return pivots[:1, :]


def factor_kernel(
    place,
    gathered,
    own,
    turned_rows,
    pivots,
    panel,
    corner,
    work,
    inverse,
    factored,
    left,
    ahead,
    block,
    reciprocals,
):
    row_block, col_block, odd = place[0], place[1], place[2]
    first = lax.broadcasted_iota(jnp.int32, (8, BLOCK), 1) < 64
    for at in range(0, 2 * 16, 2):
        for side in range(2):
            source = at + jnp.where(odd == 1, 1 - side, side)
            row = 16 * (at + side)
            corner[row : row + 16, :BLOCK] = gathered[source, :16]
            corner[row : row + 16, BLOCK:NB] = gathered[source, 16:32]
            packed = gathered[source, 32:]
            turned = pltpu.roll(packed, 64, 1)
            corner[row : row + 8, NB:] = jnp.where(first, packed, turned)
            corner[row + 8 : row + 16, NB:] = jnp.where(first, turned, packed)
    half, quarter = NB, BLOCK
    same = (lax.broadcasted_iota(jnp.int32, (BLOCK, BLOCK), 0) < 64) == (
        lax.broadcasted_iota(jnp.int32, (BLOCK, BLOCK), 1) < 64
    )
    for at in range(0, WIDTH, BLOCK):
        work[at : at + BLOCK, at : at + BLOCK] = corner[at : at + BLOCK, :BLOCK]
    for at in range(0, WIDTH, NB):
        work[at + BLOCK : at + NB, at : at + BLOCK] = jnp.where(
            same, corner[at + BLOCK : at + NB, NB:], corner[at : at + BLOCK, NB:].T
        )
    work[half + quarter :, :quarter] = corner[:quarter, BLOCK:NB].T
    work[half : half + quarter, quarter:half] = corner[quarter:half, BLOCK:NB].T
    work[half : half + quarter, :quarter] = corner[half : half + quarter, BLOCK:NB]
    work[half + quarter :, quarter:half] = corner[half + quarter :, BLOCK:NB]
    lower = lax.broadcasted_iota(jnp.int32, (BLOCK, BLOCK), 0) >= lax.broadcasted_iota(
        jnp.int32, (BLOCK, BLOCK), 1
    )
    queue = []

    def between():
        if queue:
            queue.pop(0)()

    def set_columns(at):
        columns = own[:, :, at : at + BLOCK].reshape(NB, BLOCK)
        if at > 0:
            for row in range(0, NB, BLOCK):
                ahead[row : row + BLOCK, :] = columns[row : row + BLOCK] + product(
                    own[row // 16 : (row + BLOCK) // 16, :, :at].reshape(BLOCK, at),
                    inverse[at : at + BLOCK, :at],
                    1,
                    1,
                )
        else:
            ahead[...] = columns

    def set_left(base, row, turned):
        left[row : row + BLOCK, :] = product(
            work[row : row + BLOCK, base : base + BLOCK], turned, 1, 1
        )

    def update_work(row, column, block_pivots):
        work[row : row + BLOCK, column : column + BLOCK] = work[
            row : row + BLOCK, column : column + BLOCK
        ] - product(
            left[row : row + BLOCK, :], left[column : column + BLOCK, :] / block_pivots, 1, 1
        )

    def update_inverse(base, row, scaled):
        multipliers = product(left[row : row + BLOCK, :], scaled, 1, 0)
        inverse[row : row + BLOCK, base : base + BLOCK] = -multipliers
        if base > 0:
            inverse[row : row + BLOCK, :base] = inverse[row : row + BLOCK, :base] - product(
                multipliers, inverse[base : base + BLOCK, :base], 1, 0
            )

    def set_factored(base, turned):
        part = product(ahead[...], turned, 1, 1)
        if base >= NB:
            part = jnp.where(row_block == 0, 0.0, part)
        factored[:, base : base + BLOCK] = part

    def set_turned_rows(base, scaled):
        weighed = product(factored[:, base : base + BLOCK], scaled, 1, 0)
        turned_rows[:, base : base + BLOCK] = weighed

    def add_turned_rows(base):
        turned_rows[:, :base] = turned_rows[:, :base] + product(
            turned_rows[:, base : base + BLOCK], inverse[base : base + BLOCK, :base], 1, 0
        )

    set_columns(0)
    for base in range(0, WIDTH, BLOCK):
        end = base + BLOCK
        block[...] = work[base:end, base:end]
        block_pivots = factor_block(block, reciprocals, between)
        while queue:
            between()
        pivots[:, base:end] = block_pivots
        turned = jnp.where(lower, block[...], 0.0)
        scaled = turned * reciprocals[...]
        if end < WIDTH:
            set_left(base, end, turned)
            update_work(end, end, block_pivots)
        queue.append(functools.partial(set_factored, base, turned))
        queue.append(functools.partial(set_turned_rows, base, scaled))
        if base > 0:
            queue.append(functools.partial(add_turned_rows, base))
        if end < WIDTH:
            queue.append(functools.partial(update_inverse, base, end, scaled))
        for row in range(end + BLOCK, WIDTH, BLOCK):
            queue.append(functools.partial(set_left, base, row, turned))
            for column in range(end, row + BLOCK, BLOCK):
                queue.append(functools.partial(update_work, row, column, block_pivots))
            queue.append(functools.partial(update_inverse, base, row, scaled))
        if end < WIDTH:
            queue.append(functools.partial(set_columns, end))
    while queue:
        between()
    panel[...] = factored[pl.ds(pl.multiple_of(16 * col_block, 16), 16), :]


def apply_kernel(place, matrix, across, turned_rows, complement, ordered, local, arrived):
    fetch = pltpu.make_async_copy(matrix, local, arrived)
    fetch.start()
    row_block, col_block, swapped = place[0], place[1], place[3]
    for at in range(0, 2 * 16, 2):
        for side in range(2):
            ordered[16 * (at + side) : 16 * (at + side + 1), :] = across[
                at + jnp.where(swapped == 1, 1 - side, side)
            ]
    change = product(turned_rows[...], ordered[...], 1, 1)
    fetch.wait()
    kept = (row_block >= PANELS) & (col_block >= 1)
    complement[...] = jnp.where(kept, local[...] - change, 0.0)


def pieces_kernel(place, along, pieces):
    col_block, half = place[1], place[4]
    lower = jnp.where(col_block >= 8, 1, 0)
    late = lax.rem(lax.div(col_block, 4), 2)

    def block(index):
        return along[0, :, pl.ds(pl.multiple_of(index * BLOCK, BLOCK), BLOCK)]

    within = block(2 * half + 1 - lower)
    other = pltpu.roll(within, 64, 1)
    first = lax.broadcasted_iota(jnp.int32, (8, BLOCK), 1) < 64
    packed = jnp.where(
        lower == late,
        jnp.where(first, other[:8], within[8:]),
        jnp.where(first, within[:8], other[8:]),
    )
    piece = jnp.concatenate(
        [
            block(2 * half + lower),
            block(jnp.where(half == 0, 3 - lower, lower)),
            packed,
        ],
        axis=0,
    )
    pieces[...] = jnp.broadcast_to(piece[None], pieces.shape)


def in_vmem(array):
    return pltpu.with_memory_space_constraint(array, pltpu.VMEM)


def on_device(matrix):
    smem = pl.BlockSpec(memory_space=pltpu.SMEM)
    vmem = pl.BlockSpec(memory_space=pltpu.VMEM)
    half = lax.axis_index("yh")
    row_block = lax.axis_index(PROW)
    col_block = lax.axis_index("pcol")
    depth = lax.axis_index("z")
    place = jnp.stack([row_block, col_block, depth % 2, (depth + col_block) % 2, half])
    place = place.astype(jnp.int32)
    columns = lax.axis_size("pcol")
    plane = ("yh", "pcol")
    scattered = lax.all_to_all(
        matrix.reshape(columns, -1, WIDTH), "pcol", 0, 0, tiled=True
    )[0]
    copies = jnp.broadcast_to(scattered[None], (columns, *scattered.shape))
    own = lax.all_to_all(copies, "pcol", 0, 0, tiled=True)
    along = lax.all_gather(
        scattered,
        ("z", "pcol"),
        axis_index_groups=[
            [z * columns + at + (z + side) % 2 for z in range(lax.axis_size("z"))]
            for at in range(0, columns, 2)
            for side in range(2)
        ],
    )
    pieces = pl.pallas_call(
        pieces_kernel,
        out_shape=jax.ShapeDtypeStruct((2 * columns, 40, BLOCK), jnp.float32),
        in_specs=[smem, vmem],
        out_specs=vmem,
        name="pieces",
    )(place, in_vmem(along))
    gathered = lax.all_to_all(pieces, plane, 0, 0, tiled=True)
    across = lax.all_to_all(jnp.concatenate([along, along], axis=0), plane, 0, 0, tiled=True)
    turned_rows, pivots, panel = pl.pallas_call(
        factor_kernel,
        out_shape=(
            pltpu.VMEM((NB, WIDTH), jnp.float32),
            jax.ShapeDtypeStruct((1, WIDTH), jnp.float32),
            jax.ShapeDtypeStruct((16, WIDTH), jnp.float32),
        ),
        in_specs=[smem, vmem, vmem],
        out_specs=(vmem, vmem, vmem),
        scratch_shapes=[
            pltpu.VMEM((WIDTH, NB + BLOCK), jnp.float32),
            pltpu.VMEM((WIDTH, WIDTH), jnp.float32),
            pltpu.VMEM((WIDTH, WIDTH), jnp.float32),
            pltpu.VMEM((NB, WIDTH), jnp.float32),
            pltpu.VMEM((WIDTH, BLOCK), jnp.float32),
            pltpu.VMEM((NB, BLOCK), jnp.float32),
            pltpu.VMEM((BLOCK, BLOCK), jnp.float32),
            pltpu.VMEM((BLOCK, BLOCK), jnp.float32),
        ],
        cost_estimate=pl.CostEstimate(
            flops=400_000_000, bytes_accessed=3_000_000, transcendentals=0
        ),
        name="factor",
    )(place, in_vmem(gathered), in_vmem(own))
    complement = pl.pallas_call(
        apply_kernel,
        out_shape=jax.ShapeDtypeStruct(matrix.shape, jnp.float32),
        in_specs=[smem, pl.BlockSpec(memory_space=pl.ANY), vmem, vmem],
        out_specs=vmem,
        scratch_shapes=[
            pltpu.VMEM((WIDTH, WIDTH), jnp.float32),
            pltpu.VMEM((NB, WIDTH), jnp.float32),
            pltpu.SemaphoreType.DMA(()),
        ],
        cost_estimate=pl.CostEstimate(
            flops=200_000_000, bytes_accessed=3_000_000, transcendentals=0
        ),
        name="apply",
    )(place, matrix, in_vmem(across), in_vmem(turned_rows))
    return complement, panel, pivots.reshape(WIDTH)


def solution(mesh):
    split = Mesh(mesh.devices.reshape(16, 2, mesh.shape["pcol"]), ("z", "yh", "pcol"))
    return jax.shard_map(
        on_device,
        mesh=split,
        in_specs=(P(PROW, "pcol"),),
        out_specs=(P(PROW, "pcol"), P((*PROW, "pcol"), None), P()),
        check_vma=False,
    )
```

```python
import functools

import jax
import jax.numpy as jnp
from jax import lax
from jax.experimental import pallas as pl
from jax.experimental.pallas import tpu as pltpu
from jax.sharding import Mesh
from jax.sharding import PartitionSpec as P

NB = 256
PANELS = 2
WIDTH = NB * PANELS
BLOCK = 128
STEP = 8
NEAR = 2
PROW = ("z", "yh")
HIGHEST = lax.Precision.HIGHEST


def product(left, right, left_axis, right_axis):
    return lax.dot_general(
        left,
        right,
        (((left_axis,), (right_axis,)), ((), ())),
        precision=HIGHEST,
        preferred_element_type=jnp.float32,
    )


def split(value):
    high = value.astype(jnp.bfloat16).astype(jnp.float32)
    rest = value - high
    middle = rest.astype(jnp.bfloat16).astype(jnp.float32)
    return high, middle, rest - middle


def factor_block(block, reciprocals_out, between):
    sublane = lax.broadcasted_iota(jnp.int32, (STEP, BLOCK), 0)
    lane = lax.broadcasted_iota(jnp.int32, (STEP, BLOCK), 1)

    def spread_row(value, index):
        return jnp.broadcast_to(value[index : index + 1, :], (STEP, BLOCK))

    def spread_column(value, index):
        return jnp.broadcast_to(value[:, index : index + 1], (STEP, BLOCK))

    pivots = jnp.zeros((STEP, BLOCK), jnp.float32)
    steps = BLOCK // STEP
    columns = None
    lefts, rights = [], []
    for step in range(steps):
        at = STEP * step
        even = step % 2 == 0
        near = range(1, min(NEAR + even, steps - 1 - step) + 1)
        current = (lane >= at) & (lane < at + STEP)
        rows = block[at : at + STEP, :]
        if columns is None:
            columns = [spread_column(rows, at + j) for j in range(STEP)]
        rows = jnp.where(current, jnp.where(lane == sublane + at, 1.0, 0.0), rows)
        next_rows, below, upcoming = {}, {}, []
        for group in near:
            next_rows[group] = block[at + STEP * group : at + STEP * (group + 1), :]
            below[group] = [spread_column(next_rows[group], at + j) for j in range(STEP)]
            if group == 1:
                upcoming = [spread_column(next_rows[1], at + STEP + j) for j in range(STEP)]
            next_rows[group] = jnp.where(current, 0.0, next_rows[group])
        reciprocals = jnp.zeros((STEP, BLOCK), jnp.float32)
        for k in range(STEP):
            pivot = spread_row(columns[k], k)
            reciprocal = 1.0 / pivot
            factor = jnp.where(sublane > k, columns[k] * reciprocal, 0.0)
            for j in range(k + 1, STEP):
                columns[j] = columns[j] - factor * spread_row(columns[j], k)
            pivot_row = spread_row(rows, k)
            rows = rows - factor * pivot_row
            for group in near:
                below_factor = below[group][k] * reciprocal
                if group == 1:
                    for j in range(STEP):
                        upcoming[j] = upcoming[j] - below_factor * spread_row(below[1][k], j)
                for j in range(k + 1, STEP):
                    below[group][j] = below[group][j] - below[group][k] * spread_row(factor, j)
                next_rows[group] = next_rows[group] - below_factor * pivot_row
            reciprocals = jnp.where(sublane == k, reciprocal, reciprocals)
            pivots = jnp.where(lane == at + k, pivot, pivots)
        block[at : at + STEP, :] = rows
        reciprocals_out[at : at + STEP, :] = reciprocals
        for group in near:
            block[at + STEP * group : at + STEP * (group + 1), :] = next_rows[group]
        columns = upcoming
        later = STEP * (step - step % 2 + 2 + NEAR)
        if later < BLOCK:
            a, b, c = split(rows * reciprocals)
            if even:
                rows = jnp.where((lane >= at + STEP) & (lane < at + 2 * STEP), 0.0, rows)
            d, e, f = split(rows)
            lefts += [a, a, b, b, a, c]
            rights += [d, e, d, e, f, d]
            if not even:
                change = lax.dot_general(
                    jnp.concatenate(lefts, axis=0),
                    jnp.concatenate(rights, axis=0),
                    (((0,), (0,)), ((), ())),
                    preferred_element_type=jnp.float32,
                )
                lefts, rights = [], []
                lanes = lax.broadcasted_iota(jnp.int32, (BLOCK - later, BLOCK), 1)
                block[later:, :] = (
                    jnp.where((lanes >= at - STEP) & (lanes < at + STEP), 0.0, block[later:, :])
                    - change[later:, :]
                )
        between()
    return pivots[:1, :]


def factor_kernel(
    place,
    gathered,
    own,
    turned_rows,
    pivots,
    panel,
    corner,
    work,
    inverse,
    factored,
    left,
    ahead,
    block,
    reciprocals,
):
    row_block, col_block, odd = place[0], place[1], place[2]
    first = lax.broadcasted_iota(jnp.int32, (8, BLOCK), 1) < 64
    for at in range(0, 2 * 16, 2):
        for side in range(2):
            source = at + jnp.where(odd == 1, 1 - side, side)
            row = 16 * (at + side)
            corner[row : row + 16, :BLOCK] = gathered[source, :16]
            corner[row : row + 16, BLOCK:NB] = gathered[source, 16:32]
            packed = gathered[source, 32:]
            turned = pltpu.roll(packed, 64, 1)
            corner[row : row + 8, NB:] = jnp.where(first, packed, turned)
            corner[row + 8 : row + 16, NB:] = jnp.where(first, turned, packed)
    half, quarter = NB, BLOCK
    same = (lax.broadcasted_iota(jnp.int32, (BLOCK, BLOCK), 0) < 64) == (
        lax.broadcasted_iota(jnp.int32, (BLOCK, BLOCK), 1) < 64
    )
    for at in range(0, WIDTH, BLOCK):
        work[at : at + BLOCK, at : at + BLOCK] = corner[at : at + BLOCK, :BLOCK]
    for at in range(0, WIDTH, NB):
        work[at + BLOCK : at + NB, at : at + BLOCK] = jnp.where(
            same, corner[at + BLOCK : at + NB, NB:], corner[at : at + BLOCK, NB:].T
        )
    work[half + quarter :, :quarter] = corner[:quarter, BLOCK:NB].T
    work[half : half + quarter, quarter:half] = corner[quarter:half, BLOCK:NB].T
    work[half : half + quarter, :quarter] = corner[half : half + quarter, BLOCK:NB]
    work[half + quarter :, quarter:half] = corner[half + quarter :, BLOCK:NB]
    lower = lax.broadcasted_iota(jnp.int32, (BLOCK, BLOCK), 0) >= lax.broadcasted_iota(
        jnp.int32, (BLOCK, BLOCK), 1
    )
    queue = []

    def between():
        if queue:
            queue.pop(0)()

    def set_columns(at):
        columns = own[:, :, at : at + BLOCK].reshape(NB, BLOCK)
        if at > 0:
            for row in range(0, NB, BLOCK):
                ahead[row : row + BLOCK, :] = columns[row : row + BLOCK] + product(
                    own[row // 16 : (row + BLOCK) // 16, :, :at].reshape(BLOCK, at),
                    inverse[at : at + BLOCK, :at],
                    1,
                    1,
                )
        else:
            ahead[...] = columns

    def set_left(base, row, turned):
        left[row : row + BLOCK, :] = product(
            work[row : row + BLOCK, base : base + BLOCK], turned, 1, 1
        )

    def update_work(row, column, block_pivots):
        work[row : row + BLOCK, column : column + BLOCK] = work[
            row : row + BLOCK, column : column + BLOCK
        ] - product(
            left[row : row + BLOCK, :], left[column : column + BLOCK, :] / block_pivots, 1, 1
        )

    def update_inverse(base, row, scaled):
        multipliers = product(left[row : row + BLOCK, :], scaled, 1, 0)
        inverse[row : row + BLOCK, base : base + BLOCK] = -multipliers
        if base > 0:
            inverse[row : row + BLOCK, :base] = inverse[row : row + BLOCK, :base] - product(
                multipliers, inverse[base : base + BLOCK, :base], 1, 0
            )

    def set_factored(base, turned):
        part = product(ahead[...], turned, 1, 1)
        if base >= NB:
            part = jnp.where(row_block == 0, 0.0, part)
        factored[:, base : base + BLOCK] = part

    def set_turned_rows(base, scaled):
        weighed = product(factored[:, base : base + BLOCK], scaled, 1, 0)
        turned_rows[:, base : base + BLOCK] = weighed

    def add_turned_rows(base):
        turned_rows[:, :base] = turned_rows[:, :base] + product(
            turned_rows[:, base : base + BLOCK], inverse[base : base + BLOCK, :base], 1, 0
        )

    set_columns(0)
    for base in range(0, WIDTH, BLOCK):
        end = base + BLOCK
        block[...] = work[base:end, base:end]
        block_pivots = factor_block(block, reciprocals, between)
        while queue:
            between()
        pivots[:, base:end] = block_pivots
        turned = jnp.where(lower, block[...], 0.0)
        scaled = turned * reciprocals[...]
        if end < WIDTH:
            set_left(base, end, turned)
            update_work(end, end, block_pivots)
        queue.append(functools.partial(set_factored, base, turned))
        queue.append(functools.partial(set_turned_rows, base, scaled))
        if base > 0:
            queue.append(functools.partial(add_turned_rows, base))
        if end < WIDTH:
            queue.append(functools.partial(update_inverse, base, end, scaled))
        for row in range(end + BLOCK, WIDTH, BLOCK):
            queue.append(functools.partial(set_left, base, row, turned))
            for column in range(end, row + BLOCK, BLOCK):
                queue.append(functools.partial(update_work, row, column, block_pivots))
            queue.append(functools.partial(update_inverse, base, row, scaled))
        if end < WIDTH:
            queue.append(functools.partial(set_columns, end))
    while queue:
        between()
    panel[...] = factored[pl.ds(pl.multiple_of(16 * col_block, 16), 16), :]


def apply_kernel(place, matrix, across, turned_rows, complement, ordered, local, arrived):
    fetch = pltpu.make_async_copy(matrix, local, arrived)
    fetch.start()
    row_block, col_block, swapped = place[0], place[1], place[3]
    for at in range(0, 2 * 16, 2):
        for side in range(2):
            ordered[16 * (at + side) : 16 * (at + side + 1), :] = across[
                at + jnp.where(swapped == 1, 1 - side, side)
            ]
    change = product(turned_rows[...], ordered[...], 1, 1)
    fetch.wait()
    kept = (row_block >= PANELS) & (col_block >= 1)
    complement[...] = jnp.where(kept, local[...] - change, 0.0)


def pieces_kernel(place, along, pieces, piece, sent):
    col_block, half = place[1], place[4]
    lower = jnp.where(col_block >= 8, 1, 0)
    late = lax.rem(lax.div(col_block, 4), 2)

    def block(index):
        return along[0, :, pl.ds(pl.multiple_of(index * BLOCK, BLOCK), BLOCK)]

    within = block(2 * half + 1 - lower)
    other = pltpu.roll(within, 64, 1)
    first = lax.broadcasted_iota(jnp.int32, (8, BLOCK), 1) < 64
    packed = jnp.where(
        lower == late,
        jnp.where(first, other[:8], within[8:]),
        jnp.where(first, within[:8], other[8:]),
    )
    piece[:16, :] = block(2 * half + lower)
    piece[16:32, :] = block(jnp.where(half == 0, 3 - lower, lower))
    piece[32:, :] = packed
    spread(piece, pieces, sent)


def spread(source, target, sent):
    copies = [
        pltpu.make_async_copy(source, target.at[at], sent.at[at]) for at in range(target.shape[0])
    ]
    for copy in copies:
        copy.start()
    for copy in copies:
        copy.wait()


def copies_kernel(rows, copies, sent):
    spread(rows.at[0], copies, sent)


def in_vmem(array):
    return pltpu.with_memory_space_constraint(array, pltpu.VMEM)


def on_device(matrix):
    smem = pl.BlockSpec(memory_space=pltpu.SMEM)
    vmem = pl.BlockSpec(memory_space=pltpu.VMEM)
    half = lax.axis_index("yh")
    row_block = lax.axis_index(PROW)
    col_block = lax.axis_index("pcol")
    depth = lax.axis_index("z")
    place = jnp.stack([row_block, col_block, depth % 2, (depth + col_block) % 2, half])
    place = place.astype(jnp.int32)
    columns = lax.axis_size("pcol")
    plane = ("yh", "pcol")
    scattered = lax.all_to_all(
        matrix.reshape(columns, -1, WIDTH), "pcol", 0, 0, tiled=True
    )
    copies = pl.pallas_call(
        copies_kernel,
        out_shape=jax.ShapeDtypeStruct(scattered.shape, jnp.float32),
        in_specs=[vmem],
        out_specs=pl.BlockSpec(memory_space=pl.ANY),
        scratch_shapes=[pltpu.SemaphoreType.DMA((columns,))],
        compiler_params=pltpu.CompilerParams(vmem_limit_bytes=4 << 20),
        name="copies",
    )(in_vmem(scattered))
    scattered = scattered[0]
    own = lax.all_to_all(copies, "pcol", 0, 0, tiled=True)
    along = lax.all_gather(
        scattered,
        ("z", "pcol"),
        axis_index_groups=[
            [z * columns + at + (z + side) % 2 for z in range(lax.axis_size("z"))]
            for at in range(0, columns, 2)
            for side in range(2)
        ],
    )
    pieces = pl.pallas_call(
        pieces_kernel,
        out_shape=jax.ShapeDtypeStruct((2 * columns, 40, BLOCK), jnp.float32),
        in_specs=[smem, vmem],
        out_specs=pl.BlockSpec(memory_space=pl.ANY),
        scratch_shapes=[
            pltpu.VMEM((40, BLOCK), jnp.float32),
            pltpu.SemaphoreType.DMA((2 * columns,)),
        ],
        compiler_params=pltpu.CompilerParams(vmem_limit_bytes=4 << 20),
        name="pieces",
    )(place, in_vmem(along))
    gathered = lax.all_to_all(pieces, plane, 0, 0, tiled=True)
    across = lax.all_to_all(jnp.concatenate([along, along], axis=0), plane, 0, 0, tiled=True)
    turned_rows, pivots, panel = pl.pallas_call(
        factor_kernel,
        out_shape=(
            pltpu.VMEM((NB, WIDTH), jnp.float32),
            jax.ShapeDtypeStruct((1, WIDTH), jnp.float32),
            jax.ShapeDtypeStruct((16, WIDTH), jnp.float32),
        ),
        in_specs=[smem, vmem, vmem],
        out_specs=(vmem, vmem, vmem),
        scratch_shapes=[
            pltpu.VMEM((WIDTH, NB + BLOCK), jnp.float32),
            pltpu.VMEM((WIDTH, WIDTH), jnp.float32),
            pltpu.VMEM((WIDTH, WIDTH), jnp.float32),
            pltpu.VMEM((NB, WIDTH), jnp.float32),
            pltpu.VMEM((WIDTH, BLOCK), jnp.float32),
            pltpu.VMEM((NB, BLOCK), jnp.float32),
            pltpu.VMEM((BLOCK, BLOCK), jnp.float32),
            pltpu.VMEM((BLOCK, BLOCK), jnp.float32),
        ],
        cost_estimate=pl.CostEstimate(
            flops=400_000_000, bytes_accessed=3_000_000, transcendentals=0
        ),
        name="factor",
    )(place, in_vmem(gathered), in_vmem(own))
    complement = pl.pallas_call(
        apply_kernel,
        out_shape=jax.ShapeDtypeStruct(matrix.shape, jnp.float32),
        in_specs=[smem, pl.BlockSpec(memory_space=pl.ANY), vmem, vmem],
        out_specs=vmem,
        scratch_shapes=[
            pltpu.VMEM((WIDTH, WIDTH), jnp.float32),
            pltpu.VMEM((NB, WIDTH), jnp.float32),
            pltpu.SemaphoreType.DMA(()),
        ],
        cost_estimate=pl.CostEstimate(
            flops=200_000_000, bytes_accessed=3_000_000, transcendentals=0
        ),
        name="apply",
    )(place, matrix, in_vmem(across), in_vmem(turned_rows))
    return complement, panel, pivots.reshape(WIDTH)


def solution(mesh):
    split = Mesh(mesh.devices.reshape(16, 2, mesh.shape["pcol"]), ("z", "yh", "pcol"))
    return jax.shard_map(
        on_device,
        mesh=split,
        in_specs=(P(PROW, "pcol"),),
        out_specs=(P(PROW, "pcol"), P((*PROW, "pcol"), None), P()),
        check_vma=False,
    )
```

```python
import functools

import jax
import jax.numpy as jnp
from jax import lax
from jax.experimental import pallas as pl
from jax.experimental.pallas import tpu as pltpu
from jax.sharding import Mesh
from jax.sharding import PartitionSpec as P

NB = 256
PANELS = 2
WIDTH = NB * PANELS
BLOCK = 128
STEP = 8
NEAR = 2
PROW = ("z", "yh")
HIGHEST = lax.Precision.HIGHEST


def product(left, right, left_axis, right_axis):
    return lax.dot_general(
        left,
        right,
        (((left_axis,), (right_axis,)), ((), ())),
        precision=HIGHEST,
        preferred_element_type=jnp.float32,
    )


def split(value):
    high = value.astype(jnp.bfloat16).astype(jnp.float32)
    rest = value - high
    middle = rest.astype(jnp.bfloat16).astype(jnp.float32)
    return high, middle, rest - middle


def factor_block(block, reciprocals_out, between):
    sublane = lax.broadcasted_iota(jnp.int32, (STEP, BLOCK), 0)
    lane = lax.broadcasted_iota(jnp.int32, (STEP, BLOCK), 1)

    def spread_row(value, index):
        return jnp.broadcast_to(value[index : index + 1, :], (STEP, BLOCK))

    def spread_column(value, index):
        return jnp.broadcast_to(value[:, index : index + 1], (STEP, BLOCK))

    pivots = jnp.zeros((STEP, BLOCK), jnp.float32)
    steps = BLOCK // STEP
    columns = None
    lefts, rights = [], []
    for step in range(steps):
        at = STEP * step
        even = step % 2 == 0
        near = range(1, min(NEAR + even, steps - 1 - step) + 1)
        current = (lane >= at) & (lane < at + STEP)
        rows = block[at : at + STEP, :]
        if columns is None:
            columns = [spread_column(rows, at + j) for j in range(STEP)]
        rows = jnp.where(current, jnp.where(lane == sublane + at, 1.0, 0.0), rows)
        next_rows, below, upcoming = {}, {}, []
        for group in near:
            next_rows[group] = block[at + STEP * group : at + STEP * (group + 1), :]
            below[group] = [spread_column(next_rows[group], at + j) for j in range(STEP)]
            if group == 1:
                upcoming = [spread_column(next_rows[1], at + STEP + j) for j in range(STEP)]
            next_rows[group] = jnp.where(current, 0.0, next_rows[group])
        reciprocals = jnp.zeros((STEP, BLOCK), jnp.float32)
        for k in range(STEP):
            pivot = spread_row(columns[k], k)
            reciprocal = 1.0 / pivot
            factor = jnp.where(sublane > k, columns[k] * reciprocal, 0.0)
            for j in range(k + 1, STEP):
                columns[j] = columns[j] - factor * spread_row(columns[j], k)
            pivot_row = spread_row(rows, k)
            rows = rows - factor * pivot_row
            for group in near:
                below_factor = below[group][k] * reciprocal
                if group == 1:
                    for j in range(STEP):
                        upcoming[j] = upcoming[j] - below_factor * spread_row(below[1][k], j)
                for j in range(k + 1, STEP):
                    below[group][j] = below[group][j] - below[group][k] * spread_row(factor, j)
                next_rows[group] = next_rows[group] - below_factor * pivot_row
            reciprocals = jnp.where(sublane == k, reciprocal, reciprocals)
            pivots = jnp.where(lane == at + k, pivot, pivots)
        block[at : at + STEP, :] = rows
        reciprocals_out[at : at + STEP, :] = reciprocals
        for group in near:
            block[at + STEP * group : at + STEP * (group + 1), :] = next_rows[group]
        columns = upcoming
        later = STEP * (step - step % 2 + 2 + NEAR)
        if later < BLOCK:
            a, b, c = split(rows * reciprocals)
            if even:
                rows = jnp.where((lane >= at + STEP) & (lane < at + 2 * STEP), 0.0, rows)
            d, e, f = split(rows)
            lefts += [a, a, b, b, a, c]
            rights += [d, e, d, e, f, d]
            if not even:
                change = lax.dot_general(
                    jnp.concatenate(lefts, axis=0),
                    jnp.concatenate(rights, axis=0),
                    (((0,), (0,)), ((), ())),
                    preferred_element_type=jnp.float32,
                )
                lefts, rights = [], []
                lanes = lax.broadcasted_iota(jnp.int32, (BLOCK - later, BLOCK), 1)
                block[later:, :] = (
                    jnp.where((lanes >= at - STEP) & (lanes < at + STEP), 0.0, block[later:, :])
                    - change[later:, :]
                )
        between()
    return pivots[:1, :]


def factor_kernel(
    place,
    gathered,
    own,
    turned_rows,
    pivots,
    panel,
    corner,
    work,
    inverse,
    factored,
    left,
    ahead,
    block,
    reciprocals,
):
    row_block, col_block, odd = place[0], place[1], place[2]
    first = lax.broadcasted_iota(jnp.int32, (8, BLOCK), 1) < 64
    for at in range(0, 2 * 16, 2):
        for side in range(2):
            source = at + jnp.where(odd == 1, 1 - side, side)
            row = 16 * (at + side)
            corner[row : row + 16, :BLOCK] = gathered[source, :16]
            corner[row : row + 16, BLOCK:NB] = gathered[source, 16:32]
            packed = gathered[source, 32:]
            turned = pltpu.roll(packed, 64, 1)
            corner[row : row + 8, NB:] = jnp.where(first, packed, turned)
            corner[row + 8 : row + 16, NB:] = jnp.where(first, turned, packed)
    half, quarter = NB, BLOCK
    same = (lax.broadcasted_iota(jnp.int32, (BLOCK, BLOCK), 0) < 64) == (
        lax.broadcasted_iota(jnp.int32, (BLOCK, BLOCK), 1) < 64
    )
    for at in range(0, WIDTH, BLOCK):
        work[at : at + BLOCK, at : at + BLOCK] = corner[at : at + BLOCK, :BLOCK]
    for at in range(0, WIDTH, NB):
        work[at + BLOCK : at + NB, at : at + BLOCK] = jnp.where(
            same, corner[at + BLOCK : at + NB, NB:], corner[at : at + BLOCK, NB:].T
        )
    work[half + quarter :, :quarter] = corner[:quarter, BLOCK:NB].T
    work[half : half + quarter, quarter:half] = corner[quarter:half, BLOCK:NB].T
    work[half : half + quarter, :quarter] = corner[half : half + quarter, BLOCK:NB]
    work[half + quarter :, quarter:half] = corner[half + quarter :, BLOCK:NB]
    lower = lax.broadcasted_iota(jnp.int32, (BLOCK, BLOCK), 0) >= lax.broadcasted_iota(
        jnp.int32, (BLOCK, BLOCK), 1
    )
    queue = []

    def between():
        if queue:
            queue.pop(0)()

    def set_columns(at):
        columns = own[:, :, at : at + BLOCK].reshape(NB, BLOCK)
        if at > 0:
            for row in range(0, NB, BLOCK):
                ahead[row : row + BLOCK, :] = columns[row : row + BLOCK] + product(
                    own[row // 16 : (row + BLOCK) // 16, :, :at].reshape(BLOCK, at),
                    inverse[at : at + BLOCK, :at],
                    1,
                    1,
                )
        else:
            ahead[...] = columns

    def set_left(base, row, turned):
        left[row : row + BLOCK, :] = product(
            work[row : row + BLOCK, base : base + BLOCK], turned, 1, 1
        )

    def update_work(row, column, block_pivots):
        work[row : row + BLOCK, column : column + BLOCK] = work[
            row : row + BLOCK, column : column + BLOCK
        ] - product(
            left[row : row + BLOCK, :], left[column : column + BLOCK, :] / block_pivots, 1, 1
        )

    def update_inverse(base, row, scaled):
        multipliers = product(left[row : row + BLOCK, :], scaled, 1, 0)
        inverse[row : row + BLOCK, base : base + BLOCK] = -multipliers
        if base > 0:
            inverse[row : row + BLOCK, :base] = inverse[row : row + BLOCK, :base] - product(
                multipliers, inverse[base : base + BLOCK, :base], 1, 0
            )

    def set_factored(base, turned):
        part = product(ahead[...], turned, 1, 1)
        if base >= NB:
            part = jnp.where(row_block == 0, 0.0, part)
        factored[:, base : base + BLOCK] = part

    def set_turned_rows(base, scaled):
        weighed = product(factored[:, base : base + BLOCK], scaled, 1, 0)
        turned_rows[:, base : base + BLOCK] = weighed

    def add_turned_rows(base):
        turned_rows[:, :base] = turned_rows[:, :base] + product(
            turned_rows[:, base : base + BLOCK], inverse[base : base + BLOCK, :base], 1, 0
        )

    set_columns(0)
    for base in range(0, WIDTH, BLOCK):
        end = base + BLOCK
        block[...] = work[base:end, base:end]
        block_pivots = factor_block(block, reciprocals, between)
        while queue:
            between()
        pivots[:, base:end] = block_pivots
        turned = jnp.where(lower, block[...], 0.0)
        scaled = turned * reciprocals[...]
        if end < WIDTH:
            set_left(base, end, turned)
            update_work(end, end, block_pivots)
        queue.append(functools.partial(set_factored, base, turned))
        queue.append(functools.partial(set_turned_rows, base, scaled))
        if base > 0:
            queue.append(functools.partial(add_turned_rows, base))
        if end < WIDTH:
            queue.append(functools.partial(update_inverse, base, end, scaled))
        for row in range(end + BLOCK, WIDTH, BLOCK):
            queue.append(functools.partial(set_left, base, row, turned))
            for column in range(end, row + BLOCK, BLOCK):
                queue.append(functools.partial(update_work, row, column, block_pivots))
            queue.append(functools.partial(update_inverse, base, row, scaled))
        if end < WIDTH:
            queue.append(functools.partial(set_columns, end))
    while queue:
        between()
    panel[...] = factored[pl.ds(pl.multiple_of(16 * col_block, 16), 16), :]


def apply_kernel(place, matrix, across, turned_rows, complement, ordered, local, arrived):
    fetch = pltpu.make_async_copy(matrix, local, arrived)
    fetch.start()
    row_block, col_block, swapped = place[0], place[1], place[3]
    for at in range(0, 2 * 16, 2):
        for side in range(2):
            ordered[16 * (at + side) : 16 * (at + side + 1), :] = across[
                at + jnp.where(swapped == 1, 1 - side, side)
            ]
    change = product(turned_rows[...], ordered[...], 1, 1)
    fetch.wait()
    kept = (row_block >= PANELS) & (col_block >= 1)
    complement[...] = jnp.where(kept, local[...] - change, 0.0)


def pieces_kernel(place, along, pieces):
    col_block, half = place[1], place[4]
    lower = jnp.where(col_block >= 8, 1, 0)
    late = lax.rem(lax.div(col_block, 4), 2)

    def block(index):
        return along[0, :, pl.ds(pl.multiple_of(index * BLOCK, BLOCK), BLOCK)]

    within = block(2 * half + 1 - lower)
    other = pltpu.roll(within, 64, 1)
    first = lax.broadcasted_iota(jnp.int32, (8, BLOCK), 1) < 64
    packed = jnp.where(
        lower == late,
        jnp.where(first, other[:8], within[8:]),
        jnp.where(first, within[:8], other[8:]),
    )
    piece = jnp.concatenate(
        [
            block(2 * half + lower),
            block(jnp.where(half == 0, 3 - lower, lower)),
            packed,
        ],
        axis=0,
    )
    pieces[...] = piece


def in_vmem(array):
    return pltpu.with_memory_space_constraint(array, pltpu.VMEM)


def on_device(matrix):
    smem = pl.BlockSpec(memory_space=pltpu.SMEM)
    vmem = pl.BlockSpec(memory_space=pltpu.VMEM)
    half = lax.axis_index("yh")
    row_block = lax.axis_index(PROW)
    col_block = lax.axis_index("pcol")
    depth = lax.axis_index("z")
    place = jnp.stack([row_block, col_block, depth % 2, (depth + col_block) % 2, half])
    place = place.astype(jnp.int32)
    columns = lax.axis_size("pcol")
    plane = ("yh", "pcol")
    scattered = lax.all_to_all(
        matrix.reshape(columns, -1, WIDTH), "pcol", 0, 0, tiled=True
    )[0]
    copies = jnp.broadcast_to(scattered[None], (columns, *scattered.shape))
    own = lax.all_to_all(copies, "pcol", 0, 0, tiled=True)
    along = lax.all_gather(
        scattered,
        ("z", "pcol"),
        axis_index_groups=[
            [z * columns + at + (z + side) % 2 for z in range(lax.axis_size("z"))]
            for at in range(0, columns, 2)
            for side in range(2)
        ],
    )
    pieces = pl.pallas_call(
        pieces_kernel,
        out_shape=jax.ShapeDtypeStruct((40, BLOCK), jnp.float32),
        in_specs=[smem, vmem],
        out_specs=vmem,
        compiler_params=pltpu.CompilerParams(vmem_limit_bytes=4 << 20),
        name="pieces",
    )(place, in_vmem(along))
    pieces = jnp.broadcast_to(pieces[None], (2 * columns, *pieces.shape))
    gathered = lax.all_to_all(pieces, plane, 0, 0, tiled=True)
    across = lax.all_to_all(jnp.concatenate([along, along], axis=0), plane, 0, 0, tiled=True)
    turned_rows, pivots, panel = pl.pallas_call(
        factor_kernel,
        out_shape=(
            pltpu.VMEM((NB, WIDTH), jnp.float32),
            jax.ShapeDtypeStruct((1, WIDTH), jnp.float32),
            jax.ShapeDtypeStruct((16, WIDTH), jnp.float32),
        ),
        in_specs=[smem, vmem, vmem],
        out_specs=(vmem, vmem, vmem),
        scratch_shapes=[
            pltpu.VMEM((WIDTH, NB + BLOCK), jnp.float32),
            pltpu.VMEM((WIDTH, WIDTH), jnp.float32),
            pltpu.VMEM((WIDTH, WIDTH), jnp.float32),
            pltpu.VMEM((NB, WIDTH), jnp.float32),
            pltpu.VMEM((WIDTH, BLOCK), jnp.float32),
            pltpu.VMEM((NB, BLOCK), jnp.float32),
            pltpu.VMEM((BLOCK, BLOCK), jnp.float32),
            pltpu.VMEM((BLOCK, BLOCK), jnp.float32),
        ],
        cost_estimate=pl.CostEstimate(
            flops=400_000_000, bytes_accessed=3_000_000, transcendentals=0
        ),
        name="factor",
    )(place, in_vmem(gathered), in_vmem(own))
    complement = pl.pallas_call(
        apply_kernel,
        out_shape=jax.ShapeDtypeStruct(matrix.shape, jnp.float32),
        in_specs=[smem, pl.BlockSpec(memory_space=pl.ANY), vmem, vmem],
        out_specs=vmem,
        scratch_shapes=[
            pltpu.VMEM((WIDTH, WIDTH), jnp.float32),
            pltpu.VMEM((NB, WIDTH), jnp.float32),
            pltpu.SemaphoreType.DMA(()),
        ],
        cost_estimate=pl.CostEstimate(
            flops=200_000_000, bytes_accessed=3_000_000, transcendentals=0
        ),
        name="apply",
    )(place, matrix, in_vmem(across), in_vmem(turned_rows))
    return complement, panel, pivots.reshape(WIDTH)


def solution(mesh):
    split = Mesh(mesh.devices.reshape(16, 2, mesh.shape["pcol"]), ("z", "yh", "pcol"))
    return jax.shard_map(
        on_device,
        mesh=split,
        in_specs=(P(PROW, "pcol"),),
        out_specs=(P(PROW, "pcol"), P((*PROW, "pcol"), None), P()),
        check_vma=False,
    )
```
